32 devices in a mesh: rep: 1 (over z), data: 4 (over y), model: 8 (over x, core).
Axes of the slice: x: 4, y: 4, z: 1, core: 2. Of those that a mesh axis runs over, the one named last changes fastest.
The devices are a block of a 4x4x8 slice.
Arguments:
- x_in: bfloat16 [8, 1024, 4096], P(('rep', 'data'), 'model')
- key_lens: int32 [8], P(('rep', 'data'))
- ln_gain: bfloat16 [2, 4096], P(None, 'data')
- w_in: bfloat16 [2, 4096, 38912], P(None, 'data', 'model')
- w_out_attn: bfloat16 [2, 4096, 4096], P(None, 'model', 'data')
- w_out_mlp: bfloat16 [2, 16384, 4096], P(None, 'model', 'data')
Outputs:
- output: bfloat16 [8, 1024, 4096], P(('rep', 'data'), 'model')
All inputs are finite; a program needn't handle non-finite values.
Results may differ from the reference program's by a relative error of at most 0.0171249.
Values are sent between devices in bfloat16 or wider.
A program may use at most 768 MiB of HBM per device.

```python
import jax
import jax.numpy as jnp
from jax import lax

D = 4096
HEADS = 32
HEAD = 128
FF = 16384
KV_HEADS = 8
LAYERS = 2
BATCH = 8
SEQ = 1024

Q_GROUP = HEADS // KV_HEADS
FF_GROUP = FF // KV_HEADS
Q_WIDTH = Q_GROUP * HEAD
FF_START = Q_WIDTH + 2 * HEAD
BLOCK_IN = FF_START + 2 * FF_GROUP
EPSILON = 1e-6
NEG_BIG = -1e30


def draw_lengths(len_key):
    drawn = jax.random.randint(len_key, (BATCH,), SEQ // 2, SEQ + 1, dtype=jnp.int32)
    return jnp.where(jnp.arange(BATCH) == 0, SEQ, drawn).astype(jnp.int32)


def setup_inputs(seed: int = 0, part: int = 0) -> dict:
    part_key = jax.random.fold_in(jax.random.key(seed), part)
    act_key, len_key = jax.random.split(part_key, 2)
    shared = jax.random.split(jax.random.key(seed + 1), 4)
    x_in = jax.random.normal(act_key, (BATCH, SEQ, D), jnp.float32).astype(jnp.bfloat16)
    key_lens = draw_lengths(len_key)
    ln_gain = (1.0 + 0.3 * jax.random.normal(shared[0], (LAYERS, D), jnp.float32)).astype(jnp.bfloat16)
    in_cols = jnp.arange(BLOCK_IN)
    in_scale = jnp.where(in_cols < Q_WIDTH + HEAD, 1.5, 1.0) * D ** -0.5
    w_in = (jax.random.normal(shared[1], (LAYERS, D, KV_HEADS, BLOCK_IN), jnp.float32) * in_scale).reshape(LAYERS, D, KV_HEADS * BLOCK_IN).astype(jnp.bfloat16)
    out_scale = (HEADS * HEAD + FF) ** -0.5
    w_out_attn = (2.0 * out_scale * jax.random.normal(shared[2], (LAYERS, HEADS * HEAD, D), jnp.float32)).astype(jnp.bfloat16)
    w_out_mlp = (out_scale * jax.random.normal(shared[3], (LAYERS, FF, D), jnp.float32)).astype(jnp.bfloat16)
    return {'x_in': x_in, 'key_lens': key_lens, 'ln_gain': ln_gain, 'w_in': w_in, 'w_out_attn': w_out_attn, 'w_out_mlp': w_out_mlp}


def layer_norm(act_in, gain_vec):
    act_f32 = act_in.astype(jnp.float32)
    row_mean = jnp.mean(act_f32, axis=-1, keepdims=True)
    centered = act_f32 - row_mean
    row_var = jnp.mean(centered * centered, axis=-1, keepdims=True)
    return (centered * lax.rsqrt(row_var + EPSILON) * gain_vec.astype(jnp.float32)).astype(jnp.bfloat16)


def mix_block(h_seq, key_len, w_in_l, w_attn_g, w_mlp_g):
    projected = jnp.dot(h_seq, w_in_l, preferred_element_type=jnp.float32).astype(jnp.bfloat16)
    projected = projected.reshape(SEQ, KV_HEADS, BLOCK_IN).astype(jnp.float32)
    queries = projected[:, :, :Q_WIDTH].reshape(SEQ, KV_HEADS, Q_GROUP, HEAD)
    key_heads = projected[:, :, Q_WIDTH:Q_WIDTH + HEAD]
    value_heads = projected[:, :, Q_WIDTH + HEAD:FF_START]
    gate_proj = projected[:, :, FF_START:FF_START + FF_GROUP]
    up_proj = projected[:, :, FF_START + FF_GROUP:]
    scores = jnp.einsum('qhgd,khd->hgqk', queries, key_heads) * HEAD ** -0.5
    positions = jnp.arange(SEQ)
    allowed = (positions[None, :] <= positions[:, None]) & (positions[None, :] < key_len)
    scores = jnp.where(allowed, scores, NEG_BIG)
    soft_probs = jax.nn.softmax(scores, axis=-1)
    attn_heads = jnp.einsum('hgqk,khd->qhgd', soft_probs, value_heads).astype(jnp.bfloat16).reshape(SEQ, KV_HEADS, Q_WIDTH)
    mlp_act = (jax.nn.silu(gate_proj) * up_proj).astype(jnp.bfloat16)
    group_part = (jnp.einsum('shr,hrd->hsd', attn_heads.astype(jnp.float32), w_attn_g) + jnp.einsum('shf,hfd->hsd', mlp_act.astype(jnp.float32), w_mlp_g)).astype(jnp.bfloat16)
    return jnp.sum(group_part.astype(jnp.float32), axis=0)


def reference(x_in, key_lens, ln_gain, w_in, w_out_attn, w_out_mlp):
    def layer_step(hidden, layer_weights):
        gain_vec, w_in_l, w_attn_l, w_mlp_l = layer_weights
        w_attn_g = w_attn_l.reshape(KV_HEADS, Q_WIDTH, D).astype(jnp.float32)
        w_mlp_g = w_mlp_l.reshape(KV_HEADS, FF_GROUP, D).astype(jnp.float32)

        def per_sequence(seq_args):
            x_seq, key_len = seq_args
            h_seq = layer_norm(x_seq, gain_vec)
            z_sum = mix_block(h_seq, key_len, w_in_l, w_attn_g, w_mlp_g)
            return (x_seq.astype(jnp.float32) + z_sum).astype(jnp.bfloat16)

        return lax.map(per_sequence, (hidden, key_lens)), None

    y_out, unused_stack = lax.scan(layer_step, x_in, (ln_gain, w_in, w_out_attn, w_out_mlp))
    return y_out
```

```python
import functools

import jax
import jax.numpy as jnp
from jax import lax
from jax.experimental import pallas as pl
from jax.experimental.pallas import tpu as pltpu
from jax.sharding import PartitionSpec as P

EPSILON = 1e-6
NEG_BIG = -1e30
MESH = pl.DeviceIdType.MESH
BF = jnp.bfloat16
F32 = jnp.float32
NS = 3


def kernel(cfg, x_ref, kl_ref, gain_ref, wi_ref, wa_ref, wm_ref,
           y_ref, wi_buf, wa_buf, wm_buf,
           hv, qkv, om, wv, zs, ra, rb, cst, parts, xv, hs, gfull, klb, kcur,
           w_r1, w_r2, w_d1, w_d2, w_s1, w_s2, w_s3, w_s4, wld, misc,
           g_s, g_r, k_s, k_r, ax_s, ax_r, ad_s, ad_r, rg_s, rg_r, rf_s, rf_r,
           a_s, a_r, b_s, b_r, c_s, pd_r, pa_r, free_sem):
    (n_data, n_x, nb, sl, dm, dloc, qw, hd, ff, nl) = cfg
    seq = sl * 2 * n_x
    blk = 2 * sl
    cw = 512
    hw = cw // 2
    kv0 = qw
    ff0 = qw + 2 * hd
    n_gu = ff // hw
    n_in = 2 + n_gu
    n_out = dloc // cw
    n_u = n_in + n_out
    n_t = n_data * n_out
    rw = qw + ff

    d = lax.axis_index('data')
    m = lax.axis_index('model')
    x = lax.div(m, 2)
    c = lax.rem(m, 2)
    d_odd = lax.rem(d, 2)
    nbr1 = d + 1 - 2 * d_odd
    nbr3 = n_data - 1 - d
    opp = lax.rem(d + 2, n_data)
    xr = lax.rem(x + 1, n_x)
    xl = lax.rem(x + n_x - 1, n_x)
    xo = lax.rem(x + 2, n_x)

    def dev(dd, xx, cc):
        return {'data': dd, 'model': xx * 2 + cc}

    def rc(src, dst, ss, rs, to):
        return pltpu.make_async_remote_copy(src_ref=src, dst_ref=dst, send_sem=ss, recv_sem=rs, device_id=to, device_id_type=MESH)

    other = dev(d, x, 1 - c)
    right = dev(d, xr, c)
    left = dev(d, xl, c)

    class Lay:
        pass

    lays = []
    for l in range(nl):
        L = Lay()
        L.l = l
        if l % 2 == 0:
            L.p, L.q, a = nbr1, nbr3, lax.div(d, 2)
        else:
            L.p, L.q, a = nbr3, nbr1, lax.rem(lax.div(d + 1, 2), 2)
        L.isb = (c - a) * (c - a)
        L.src1 = L.p + (L.q - L.p) * L.isb
        L.srcx = L.q + (L.p - L.q) * L.isb
        L.src2 = opp + (d - opp) * L.isb
        L.first = dev(L.src1, x, c + (1 - 2 * c) * L.isb)
        L.pair = dev(L.p, x, c)
        lays.append(L)

    barrier = pltpu.get_barrier_semaphore()
    friends = [other, right, left, dev(nbr1, x, 0), dev(nbr1, x, 1), dev(nbr3, x, 0), dev(nbr3, x, 1), dev(opp, x, c)]
    for f in friends:
        pl.semaphore_signal(barrier, inc=1, device_id=f, device_id_type=MESH)
    xload = pltpu.make_async_copy(x_ref, xv, misc.at[0])
    xload.start()
    pl.semaphore_wait(barrier, len(friends))

    def cols(start, width):
        return pl.ds(start if isinstance(start, int) else pl.multiple_of(start, 128), width)

    class Unit:
        def __init__(self, L, s, parts_):
            self.L, self.idx, self.parts = L, (L.l * n_u + s) * 2, parts_

    def unit_in(L, s):
        l = L.l
        if isinstance(s, int) and s == 0:
            spans = [(0, qw)]
        elif isinstance(s, int) and s == 1:
            spans = [(kv0, 2 * hd)]
        else:
            k = s - 2
            spans = [(ff0 + hw * k, hw), (ff0 + ff + hw * k, hw)]
        return Unit(L, s, [(wi_ref.at[l, :, cols(c0, w)], functools.partial(lambda c0, w, e: wi_buf.at[l, e, :, cols(c0, w)], c0, w))
                           for c0, w in spans])

    def unit_out(L, v):
        l = L.l
        cc = cols(v * cw, cw)
        return Unit(L, n_in + v, [(wa_ref.at[l, :, cc], lambda e: wa_buf.at[l, e, :, cc]), (wm_ref.at[l, :, cc], lambda e: wm_buf.at[l, e, :, cc])])

    def send_own(u, cond=None):
        L = u.L

        def go():
            for i, (own, buf) in enumerate(u.parts):
                rc(own, buf(d), w_s1.at[u.idx + i], w_r1.at[u.idx + i], L.first).start()

        def go2():
            for i, (own, buf) in enumerate(u.parts):
                rc(own, buf(d), w_s3.at[u.idx + i], w_d2.at[u.idx + i], other).start()

        if cond is None or cond == 'a':
            @pl.when(L.isb == 0)
            def _():
                go2()
        if cond is None:
            go()
        else:
            @pl.when(L.isb == (0 if cond == 'a' else 1))
            def _():
                go()

    def fwd1(u):
        L = u.L
        for i, (own, buf) in enumerate(u.parts):
            rc(own, buf(L.src1), w_s1.at[u.idx + i], w_r1.at[u.idx + i], L.first).wait_recv()
            rc(buf(L.src1), buf(L.src1), w_s2.at[u.idx + i], w_d1.at[u.idx + i], other).start()

            @pl.when(L.isb == 1)
            def _():
                rc(buf(L.src1), buf(L.src1), w_s4.at[u.idx + i], w_r2.at[u.idx + i], L.pair).start()

    def fwd2(u):
        L = u.L

        @pl.when(L.isb == 1)
        def _():
            for i, (own, buf) in enumerate(u.parts):
                rc(own, buf(opp), w_s4.at[u.idx + i], w_r2.at[u.idx + i], L.pair).wait_recv()
                rc(buf(opp), buf(opp), w_s3.at[u.idx + i], w_d2.at[u.idx + i], other).start()

    def got1(u):
        for i, (own, buf) in enumerate(u.parts):
            rc(own, buf(u.L.srcx), w_s2.at[u.idx + i], w_d1.at[u.idx + i], other).wait_recv()

    def got2(u):
        for i, (own, buf) in enumerate(u.parts):
            rc(own, buf(u.L.src2), w_s3.at[u.idx + i], w_d2.at[u.idx + i], other).wait_recv()

    def sends_done(u):
        L = u.L
        for i, (own, buf) in enumerate(u.parts):
            rc(own, buf(d), w_s1.at[u.idx + i], w_r1.at[u.idx + i], L.first).wait_send()
            rc(own, buf(d), w_s2.at[u.idx + i], w_d1.at[u.idx + i], other).wait_send()
            rc(own, buf(d), w_s3.at[u.idx + i], w_d2.at[u.idx + i], other).wait_send()

            @pl.when(L.isb == 1)
            def _():
                rc(own, buf(d), w_s4.at[u.idx + i], w_r2.at[u.idx + i], L.pair).wait_send()

    def load_in(u, slot):
        L = u.L
        off = 0
        for own, buf in u.parts:
            w = own.shape[-1]

            def to(e):
                return wv.at[slot, pl.ds(pl.multiple_of(e * dloc, dloc), dloc), pl.ds(off, w)]

            for e in (L.p, L.q, opp):
                pltpu.make_async_copy(buf(e), to(e), wld.at[slot]).start()

            @pl.when(L.isb == 0)
            def _():
                pltpu.make_async_copy(own, to(d), wld.at[slot]).start()

            @pl.when(L.isb == 1)
            def _():
                pltpu.make_async_copy(buf(d), to(d), wld.at[slot]).start()
            off += w

    def wait_in(slot, w):
        pltpu.make_async_copy(wv.at[slot, :, pl.ds(0, w)], wv.at[slot, :, pl.ds(0, w)], wld.at[slot]).wait()

    def z_src(L, t):
        k, v = lax.div(t, n_out), lax.rem(t, n_out)
        src = jnp.where(k == 0, d, jnp.where(k == 1, L.q, jnp.where(k == 2, L.p, opp)))
        return k, v, src

    def z_col(L, t):
        _, v, src = z_src(L, t)
        return src * n_out + v

    def load_out(L, t, slot):
        k, v, src = z_src(L, t)
        u = unit_out(L, v)
        spots = (wv.at[slot, pl.ds(0, qw), :], wv.at[slot, pl.ds(qw, ff), :])
        mine = jnp.logical_and(k == 0, L.isb == 0)

        @pl.when(mine)
        def _():
            for (own, buf), to in zip(u.parts, spots):
                pltpu.make_async_copy(own, to, wld.at[slot]).start()

        @pl.when(jnp.logical_not(mine))
        def _():
            for (own, buf), to in zip(u.parts, spots):
                pltpu.make_async_copy(buf(src), to, wld.at[slot]).start()

    def wait_out(slot):
        ref = wv.at[slot, pl.ds(0, rw), :]
        pltpu.make_async_copy(ref, ref, wld.at[slot]).wait()

    def out_arrives(L, t):
        k, v, src = z_src(L, t)
        u = unit_out(L, v)

        @pl.when(jnp.logical_and(k == 0, L.isb == 1))
        def _():
            got2(u)

        @pl.when(jnp.logical_and(k == 1, L.isb == 0))
        def _():
            got1(u)

        @pl.when(jnp.logical_and(k == 2, L.isb == 0))
        def _():
            fwd1(u)

        @pl.when(jnp.logical_and(k == 2, L.isb == 1))
        def _():
            got1(u)

        @pl.when(k == 3)
        def _():
            fwd2(u)

        @pl.when(jnp.logical_and(k == 3, L.isb == 0))
        def _():
            got2(u)

    rows = 32

    def layer_norm(L, b):
        g = gfull[L.l, 0:1, :]

        def tile(i, _):
            r = pl.ds(pl.multiple_of(i * rows, rows), rows)
            v = xv[b, r, :].astype(F32)
            cen = v - jnp.mean(v, axis=-1, keepdims=True)
            var = jnp.mean(cen * cen, axis=-1, keepdims=True)
            h = (cen * lax.rsqrt(var + EPSILON) * g).astype(BF)
            hs[b, r, :] = h

            @pl.when(c == 0)
            def _():
                hv[b, pl.ds(pl.multiple_of(m * sl + i * rows, rows), rows), :] = h
            return 0

        lax.fori_loop(0, sl // rows, tile, 0)

    def my_rows(b):
        return hv.at[b, pl.ds(pl.multiple_of(m * sl, sl), sl), :]

    def block(b, xx, lo=0, n=None):
        return hv.at[b, pl.ds(pl.multiple_of(xx * blk, blk), blk), pl.ds(lo, dm if n is None else n)]

    def ax(L, b):
        i = L.l * nb + b
        return rc(hs.at[b], my_rows(b), ax_s.at[i], ax_r.at[2 * i + c], dev(L.q, x, 1))

    def ad(L, b):
        i = L.l * nb + b
        return rc(hs.at[b], my_rows(b), ad_s.at[i], ad_r.at[i], other)

    def share(L, b):
        ax(L, b).start()

        @pl.when(c == 1)
        def _():
            ad(L, b).start()

    def ring(L, b, way):
        i = 2 * (L.l * nb + b) + way
        return rc(block(b, x), block(b, x), rg_s.at[i], rg_r.at[i], right if way == 0 else left)

    def ring_in(L, b, way):
        i = 2 * (L.l * nb + b) + way
        src = block(b, xl if way == 0 else xr)
        return rc(src, src, rg_s.at[i], rg_r.at[i], right if way == 0 else left)

    def ring2(L, b, way, xx):
        i = 2 * (L.l * nb + b) + way
        src = block(b, xx, 0 if way == 0 else dm // 2, dm // 2)
        return rc(src, src, rf_s.at[i], rf_r.at[i], right if way == 0 else left)

    def ring_start(L, b):
        i = L.l * nb + b

        @pl.when(c == 0)
        def _():
            dst = hv.at[b, pl.ds(pl.multiple_of(x * blk + sl, sl), sl), :]
            rc(hs.at[b], dst, ad_s.at[i], ad_r.at[i], other).wait_recv()

        @pl.when(c == 1)
        def _():
            for cc in range(2):
                dst = hv.at[b, pl.ds(pl.multiple_of(x * blk + cc * sl, sl), sl), :]
                rc(hs.at[b], dst, ax_s.at[i], ax_r.at[2 * i + cc], other).wait_recv()
        for way in range(2):
            ring(L, b, way).start()

    def ring_pass(L, b):
        for way in range(2):
            ring_in(L, b, way).wait_recv()
            ring2(L, b, way, xl if way == 0 else xr).start()

    def ring_end(L, b):
        for way in range(2):
            ring2(L, b, way, xo).wait_recv()

    def gather_sends_done(L, b):
        ax(L, b).wait_send()

        @pl.when(c == 1)
        def _():
            ad(L, b).wait_send()
        for way in range(2):
            ring(L, b, way).wait_send()
            ring2(L, b, way, xl if way == 0 else xr).wait_send()

    def p_q(b, slot):
        qkv[b, :, 0:qw] = jnp.dot(hv[b], wv[slot], preferred_element_type=F32).astype(BF)

    def p_kv(b, slot):
        qkv[b, :, qw:qw + 2 * hd] = jnp.dot(hv[b], wv[slot, :, 0:2 * hd], preferred_element_type=F32).astype(BF)

    def p_gu(b, slot, k):
        acc = jnp.dot(hv[b], wv[slot], preferred_element_type=F32)
        g = acc[:, 0:hw].astype(BF).astype(F32)
        up = acc[:, hw:cw].astype(BF).astype(F32)
        om[b, :, cols(qw + hw * k, hw)] = (g * (1.0 / (1.0 + jnp.exp(-g))) * up).astype(BF)

    def attention(b):
        tq = 256
        kl = kcur[b, 0:1, 0:1]
        for i in range(seq // tq):
            n = tq * (i + 1)
            row = lax.broadcasted_iota(jnp.int32, (tq, n), 0) + tq * i
            col = lax.broadcasted_iota(jnp.int32, (tq, n), 1)
            ok = jnp.logical_and(col <= row, col < kl)

            def head(h, _):
                hc = pl.ds(pl.multiple_of(h * hd, hd), hd)
                qh = qkv[b, tq * i:tq * (i + 1), hc]
                s = lax.dot_general(qh, qkv[b, 0:n, kv0:kv0 + hd], (((1,), (1,)), ((), ())), preferred_element_type=F32) * hd ** -0.5
                s = jnp.where(ok, s, NEG_BIG)
                e = jnp.exp(s - jnp.max(s, axis=-1, keepdims=True))
                tot = jnp.sum(e, axis=-1, keepdims=True)
                o = jnp.dot(e.astype(BF), qkv[b, 0:n, kv0 + hd:kv0 + 2 * hd], preferred_element_type=F32)
                om[b, tq * i:tq * (i + 1), hc] = (o / tot).astype(BF)
                return 0

            lax.fori_loop(0, qw // hd, head, 0)

    def zblk(slot, xx, lo, n):
        return zs.at[slot, pl.ds(pl.multiple_of(xx * blk, blk), blk), pl.ds(lo, n)]

    def a_send(slot, way):
        return rc(zblk(slot, xo, way * hw, hw), ra.at[slot, way], a_s.at[2 * slot + way], a_r.at[2 * slot + way], right if way == 0 else left)

    def b_send(slot, way):
        return rc(zblk(slot, xr if way == 0 else xl, 0, cw), rb.at[slot, way], b_s.at[2 * slot + way], b_r.at[2 * slot + way],
                  right if way == 0 else left)

    def z_step(b, wslot, j):
        slot = lax.rem(j, NS)

        @pl.when(j >= NS)
        def _():
            for way in range(2):
                a_send(slot, way).wait_send()
                b_send(slot, way).wait_send()
        zs[slot] = jnp.dot(om[b], wv[wslot, 0:rw, :], preferred_element_type=F32).astype(BF)
        for way in range(2):
            a_send(slot, way).start()

    def rs_b(j):
        slot = lax.rem(j, NS)
        for way in range(2):
            a_send(slot, way).wait_recv()
            r = pl.ds(pl.multiple_of((xr if way == 0 else xl) * blk, blk), blk)
            cc = pl.ds(way * hw, hw)
            zs[slot, r, cc] = (zs[slot, r, cc].astype(F32) + ra[slot, way].astype(F32)).astype(BF)
        for way in range(2):
            b_send(slot, way).start()

    def c_send(L, b, n, slot, cc, home):
        i = (L.l * n_t + n) * nb + b
        sem = c_s.at[2 * slot + cc]
        if home:
            return rc(cst.at[slot, pl.ds(cc * sl, sl), :], parts.at[0, b, :, cols(n * cw, cw)], sem, pd_r.at[i], other)
        return rc(cst.at[slot, pl.ds(cc * sl, sl), :], parts.at[1, b, :, cols(n * cw, cw)], sem, pa_r.at[i], dev(L.q, x, cc))

    def c_wait(L, slot):
        @pl.when(c == 1)
        def _():
            for cc in range(2):
                c_send(L, 0, 0, slot, cc, False).wait_send()

        @pl.when(c == 0)
        def _():
            c_send(L, 0, 0, slot, 1, True).wait_send()

    def rs_c(L, j, b, t):
        slot = lax.rem(j, NS)
        n = z_col(L, t)
        for way in range(2):
            b_send(slot, way).wait_recv()

        @pl.when(j >= NS)
        def _():
            c_wait(L, slot)
        r = pl.ds(pl.multiple_of(x * blk, blk), blk)
        cst[slot] = (zs[slot, r, :].astype(F32) + rb[slot, 0].astype(F32) + rb[slot, 1].astype(F32)).astype(BF)

        @pl.when(c == 0)
        def _():
            c_send(L, b, n, slot, 1, True).start()
            parts[0, b, :, cols(n * cw, cw)] = cst[slot, 0:sl, :]

        @pl.when(c == 1)
        def _():
            for cc in range(2):
                c_send(L, b, n, slot, cc, False).start()

    def combine(L, b):
        for n in range(n_t):
            c_send(L, b, n, 0, 0, False).wait_recv()

            @pl.when(c == 1)
            def _():
                c_send(L, b, n, 0, 0, True).wait_recv()

        def tile(i, _):
            r = pl.ds(pl.multiple_of(i * rows, rows), rows)
            z = parts[0, b, r, :].astype(F32) + parts[1, b, r, :].astype(F32)
            xv[b, r, :] = (xv[b, r, :].astype(F32) + z).astype(BF)
            return 0

        lax.fori_loop(0, sl // rows, tile, 0)

    L0, L1 = lays
    send_own(unit_in(L0, 0))
    send_own(unit_in(L0, 1))
    g_to = [dev(nbr1, x, c), dev(nbr3, x, c), dev(opp, x, c)]

    def gsl(e):
        return gfull.at[:, :, pl.ds(pl.multiple_of(e * dloc, dloc), dloc)]

    for i in range(3):
        rc(gain_ref, gsl(d), g_s.at[i], g_r.at[i], g_to[i]).start()

    @pl.when(c == 1)
    def _():
        for l, L in enumerate(lays):
            rc(kl_ref, klb.at[l], k_s.at[l], k_r.at[l], dev(L.q, x, 1)).start()
    gfull[:, :, pl.ds(pl.multiple_of(d * dloc, dloc), dloc)] = gain_ref[...]

    def set_len(L):
        @pl.when(c == 0)
        def _():
            kcur[...] = kl_ref[...]

        @pl.when(c == 1)
        def _():
            rc(kl_ref, klb.at[L.l], k_s.at[L.l], k_r.at[L.l], other).wait_recv()
            kcur[...] = klb[L.l]

    set_len(L0)
    xload.wait()
    for i, e in enumerate((nbr1, nbr3, opp)):
        rc(gain_ref, gsl(e), g_s.at[i], g_r.at[i], g_to[i]).wait_recv()
    for b in range(nb):
        layer_norm(L0, b)
        share(L0, b)
    for s in range(2, n_in):
        send_own(unit_in(L0, s))
    for v in range(n_out):
        send_own(unit_out(L0, v))
    for b in range(nb):
        ring_start(L0, b)
    for s in range(3):
        fwd1(unit_in(L0, s))
    for b in range(nb):
        ring_pass(L0, b)

    def in_ready(L, s):
        u = unit_in(L, s)
        fwd2(u)
        got1(u)
        got2(u)

    for s in range(1):
        in_ready(L0, s)
        load_in(unit_in(L0, s), 0)
    for b in range(nb):
        ring_end(L0, b)

    def both(fn):
        def body(b, _):
            fn(b)
            return 0
        lax.fori_loop(0, nb, body, 0)

    fwd1(unit_in(L0, 3))
    in_ready(L0, 1)
    load_in(unit_in(L0, 1), 1)
    wait_in(0, cw)
    both(lambda b: p_q(b, 0))
    fwd1(unit_in(L0, 4))
    in_ready(L0, 2)
    load_in(unit_in(L0, 2), 0)
    wait_in(1, 2 * hd)
    both(lambda b: p_kv(b, 1))
    both(attention)

    def gu_loop0(k, _):
        s = k + 2
        slot = lax.rem(k, 2)

        @pl.when(s + 3 < n_in)
        def _():
            fwd1(unit_in(L0, s + 3))

        @pl.when(jnp.logical_and(jnp.logical_and(s + 3 >= n_in, s + 3 < n_u), L0.isb == 1))
        def _():
            fwd1(unit_out(L0, s + 3 - n_in))

        @pl.when(s + 1 < n_in)
        def _():
            in_ready(L0, s + 1)
            load_in(unit_in(L0, s + 1), 1 - slot)

        @pl.when(s + 1 == n_in)
        def _():
            out_arrives(L0, 0)
            load_out(L0, 0, 1 - slot)
        wait_in(slot, cw)
        both(lambda b: p_gu(b, slot, k))

        @pl.when(k >= n_gu // 2)
        def _():
            u = k - n_gu // 2

            @pl.when(u >= 2)
            def _():
                send_own(unit_in(L1, u), 'a')
        return 0

    lax.fori_loop(0, n_gu, gu_loop0, 0)
    send_own(unit_in(L1, 0), 'a')
    send_own(unit_in(L1, 1), 'a')
    for b in range(nb):
        gather_sends_done(L0, b)
    @pl.when(c == 1)
    def _():
        for cc in range(2):
            pl.semaphore_signal(free_sem, inc=1, device_id=dev(L1.q, x, cc), device_id_type=MESH)
    z0 = lax.rem(n_gu, 2)

    def z_loop0(t, _):
        wslot = lax.rem(t + z0, 2)
        wait_out(wslot)
        for b in range(nb):
            j = nb * t + b
            z_step(b, wslot, j)

            @pl.when(j >= 1)
            def _():
                rs_b(j - 1)

            @pl.when(j >= 2)
            def _():
                rs_c(L0, j - 2, b, t - 1)
            if b == 0:
                @pl.when(t + 1 < n_t)
                def _():
                    out_arrives(L0, t + 1)
                    load_out(L0, t + 1, 1 - wslot)

                @pl.when(t + 4 < n_in)
                def _():
                    send_own(unit_in(L1, t + 4), 'a')
        return 0

    lax.fori_loop(0, n_t, z_loop0, 0)
    j_end = nb * n_t
    for s in range(2):
        send_own(unit_in(L1, s), 'b')
    rs_b(j_end - 1)
    rs_c(L0, j_end - 2, 0, n_t - 1)
    rs_c(L0, j_end - 1, 1, n_t - 1)

    def layer_sends_done(L):
        sends_done(unit_in(L, 0))
        sends_done(unit_in(L, 1))

        def body(s, _):
            sends_done(unit_in(L, s))
            return 0
        lax.fori_loop(2, n_in, body, 0)

        def body2(v, _):
            sends_done(unit_out(L, v))
            return 0
        lax.fori_loop(0, n_out, body2, 0)

    pl.semaphore_wait(free_sem, 1)
    for b in range(nb):
        combine(L0, b)
        layer_norm(L1, b)
        share(L1, b)
    set_len(L1)
    for s in range(2, n_in):
        send_own(unit_in(L1, s), 'b')
    for v in range(n_out):
        send_own(unit_out(L1, v))
    ring_start(L1, 0)
    fwd1(unit_in(L1, 0))
    fwd1(unit_in(L1, 1))
    ring_start(L1, 1)
    fwd1(unit_in(L1, 2))
    ring_pass(L1, 0)
    fwd1(unit_in(L1, 3))
    in_ready(L1, 0)
    load_in(unit_in(L1, 0), 0)
    in_ready(L1, 1)
    load_in(unit_in(L1, 1), 1)
    ring_end(L1, 0)
    wait_in(0, cw)
    p_q(0, 0)
    fwd1(unit_in(L1, 4))
    in_ready(L1, 2)
    load_in(unit_in(L1, 2), 0)
    wait_in(1, 2 * hd)
    p_kv(0, 1)
    ring_pass(L1, 1)
    attention(0)

    def gu_loop1(k, _):
        s = k + 2
        slot = lax.rem(k, 2)

        @pl.when(s + 3 < n_in)
        def _():
            fwd1(unit_in(L1, s + 3))

        @pl.when(jnp.logical_and(jnp.logical_and(s + 3 >= n_in, s + 3 < n_u), L1.isb == 1))
        def _():
            fwd1(unit_out(L1, s + 3 - n_in))

        @pl.when(s + 1 < n_in)
        def _():
            in_ready(L1, s + 1)
            load_in(unit_in(L1, s + 1), 1 - slot)
        wait_in(slot, cw)
        p_gu(0, slot, k)
        return 0

    lax.fori_loop(0, n_gu, gu_loop1, 0)
    load_in(unit_in(L1, 0), 0)
    load_in(unit_in(L1, 1), 1)
    ring_end(L1, 1)
    wait_in(0, cw)
    p_q(1, 0)
    load_in(unit_in(L1, 2), 0)
    wait_in(1, 2 * hd)
    p_kv(1, 1)
    out_arrives(L1, 0)
    load_out(L1, 0, 1)
    attention(1)

    def fused(k, _):
        wait_in(0, cw)
        p_gu(1, 0, k)

        @pl.when(k + 1 < n_gu)
        def _():
            load_in(unit_in(L1, k + 3), 0)

        @pl.when(k + 1 == n_gu)
        def _():
            load_out(L1, 0, 0)
        wait_out(1)
        j = j_end + k
        z_step(0, 1, j)

        @pl.when(k >= 1)
        def _():
            rs_b(j - 1)

        @pl.when(k >= 2)
        def _():
            rs_c(L1, j - 2, 0, k - 2)

        @pl.when(k + 1 < n_t)
        def _():
            out_arrives(L1, k + 1)
            load_out(L1, k + 1, 1)
        return 0

    assert n_gu == n_t
    lax.fori_loop(0, n_t, fused, 0)
    for b in range(nb):
        gather_sends_done(L1, b)

    def z_loop1(t, _):
        wslot = lax.rem(t, 2)
        wait_out(wslot)

        @pl.when(t + 1 < n_t)
        def _():
            load_out(L1, t + 1, 1 - wslot)
        j = j_end + n_t + t
        z_step(1, wslot, j)
        rs_b(j - 1)
        i2 = n_t + t - 2
        rs_c(L1, j - 2, lax.div(i2, n_t), lax.rem(i2, n_t))
        return 0

    lax.fori_loop(0, n_t, z_loop1, 0)
    j_last = 2 * j_end - 1
    rs_b(j_last)
    rs_c(L1, j_last - 1, 1, n_t - 2)
    rs_c(L1, j_last, 1, n_t - 1)
    for b in range(nb):
        combine(L1, b)
    yout = pltpu.make_async_copy(xv, y_ref, misc.at[0])
    yout.start()
    layer_sends_done(L0)
    layer_sends_done(L1)
    for i in range(3):
        rc(gain_ref, gsl(d), g_s.at[i], g_r.at[i], g_to[i]).wait_send()

    @pl.when(c == 1)
    def _():
        for l in range(nl):
            rc(kl_ref, klb.at[l], k_s.at[l], k_r.at[l], other).wait_send()
    for slot in range(NS):
        c_wait(L1, slot)
        for way in range(2):
            a_send(slot, way).wait_send()
            b_send(slot, way).wait_send()
    yout.wait()


def solution(mesh):
    n_data = mesh.shape['data']
    n_x = mesh.shape['model'] // 2
    batch_axes = ('rep', 'data')

    def device_step(x_loc, len_loc, gain_loc, w_in_loc, w_attn_loc, w_mlp_loc):
        nl, dloc, block_in = w_in_loc.shape
        qw, ff = w_attn_loc.shape[1], w_mlp_loc.shape[1]
        hd = (block_in - qw - 2 * ff) // 2
        nb, sl, dm = x_loc.shape
        seq = sl * 2 * n_x
        cfg = (n_data, n_x, nb, sl, dm, dloc, qw, hd, ff, nl)
        cw = 512
        n_u = 2 + ff // (cw // 2) + dloc // cw
        n_t = n_data * (dloc // cw)
        lens = jnp.broadcast_to(len_loc[:, None, None], (nb, 8, 128))
        gain = jnp.broadcast_to(gain_loc.astype(F32)[:, None, :], (nl, 8, dloc))
        anyspec = pl.BlockSpec(memory_space=pl.ANY)
        vspec = pl.BlockSpec(memory_space=pltpu.VMEM)
        sem = pltpu.SemaphoreType.DMA
        out = pl.pallas_call(
            functools.partial(kernel, cfg),
            out_shape=[
                jax.ShapeDtypeStruct((nb, sl, dm), BF),
                jax.ShapeDtypeStruct((nl, n_data, dloc, block_in), BF),
                jax.ShapeDtypeStruct((nl, n_data, qw, dloc), BF),
                jax.ShapeDtypeStruct((nl, n_data, ff, dloc), BF),
            ],
            in_specs=[anyspec, vspec, vspec, anyspec, anyspec, anyspec],
            out_specs=[anyspec] * 4,
            scratch_shapes=[
                pltpu.VMEM((nb, seq, dm), BF),
                pltpu.VMEM((nb, seq, qw + 2 * hd), BF),
                pltpu.VMEM((nb, seq, qw + ff), BF),
                pltpu.VMEM((2, dm, cw), BF),
                pltpu.VMEM((NS, seq, cw), BF),
                pltpu.VMEM((NS, 2, 2 * sl, cw // 2), BF),
                pltpu.VMEM((NS, 2, 2 * sl, cw), BF),
                pltpu.VMEM((NS, 2 * sl, cw), BF),
                pltpu.VMEM((2, nb, sl, dm), BF),
                pltpu.VMEM((nb, sl, dm), BF),
                pltpu.VMEM((nb, sl, dm), BF),
                pltpu.VMEM((nl, 8, dm), F32),
                pltpu.VMEM((nl, nb, 8, 128), jnp.int32),
                pltpu.VMEM((nb, 8, 128), jnp.int32),
            ] + [sem((nl * n_u * 2,))] * 8 + [
                sem((2,)),
                sem((1,)),
                sem((3,)), sem((3,)),
                sem((nl,)), sem((nl,)),
                sem((nl * nb,)), sem((nl * nb * 2,)),
                sem((nl * nb,)), sem((nl * nb,)),
                sem((nl * nb * 2,)), sem((nl * nb * 2,)),
                sem((nl * nb * 2,)), sem((nl * nb * 2,)),
                sem((NS * 2,)), sem((NS * 2,)), sem((NS * 2,)), sem((NS * 2,)), sem((NS * 2,)),
                sem((nl * n_t * nb,)), sem((nl * n_t * nb,)),
                pltpu.SemaphoreType.REGULAR,
            ],
            compiler_params=pltpu.CompilerParams(collective_id=0, has_side_effects=True, vmem_limit_bytes=63 * 1024 * 1024),
        )(x_loc, lens, gain, w_in_loc, w_attn_loc, w_mlp_loc)
        return out[0]

    return jax.shard_map(device_step, mesh=mesh, in_specs=(P(batch_axes, 'model', None), P(batch_axes), P(None, 'data'), P(None, 'data', 'model'), P(None, 'model', 'data'), P(None, 'model', 'data')), out_specs=P(batch_axes, 'model', None), check_vma=False)
```

```python
import functools

import jax
import jax.numpy as jnp
from jax import lax
from jax.experimental import pallas as pl
from jax.experimental.pallas import tpu as pltpu
from jax.sharding import PartitionSpec as P

EPSILON = 1e-6
NEG_BIG = -1e30
MESH = pl.DeviceIdType.MESH
BF = jnp.bfloat16
F32 = jnp.float32
NS = 3
NC = 4


def kernel(cfg, x_ref, kl_ref, gain_ref, wi_ref, wa_ref, wm_ref,
           y_ref, wi_buf, wa_buf, wm_buf,
           hv, qkv, om, wv, wz, zs, ra, rb, cst, parts, xv, hs, gfull, klb, kcur,
           w_r1, w_r2, w_d1, w_d2, w_s1, w_s2, w_s3, w_s4, wld, wzs, misc,
           g_s, g_r, k_s, k_r, ax_s, ax_r, ad_s, ad_r, rg_s, rg_r, rf_s, rf_r,
           a_s, a_r, b_s, b_r, c_s, pd_r, pa_r, free_sem):
    (n_data, n_x, nb, sl, dm, dloc, qw, hd, ff, nl) = cfg
    seq = sl * 2 * n_x
    blk = 2 * sl
    cw = 512
    hw = cw // 2
    kv0 = qw
    ff0 = qw + 2 * hd
    n_gu = ff // hw
    n_in = 2 + n_gu
    n_out = dloc // cw
    n_u = n_in + n_out
    n_t = n_data * n_out
    rw = qw + ff

    d = lax.axis_index('data')
    m = lax.axis_index('model')
    x = lax.div(m, 2)
    c = lax.rem(m, 2)
    d_odd = lax.rem(d, 2)
    nbr1 = d + 1 - 2 * d_odd
    nbr3 = n_data - 1 - d
    opp = lax.rem(d + 2, n_data)
    xr = lax.rem(x + 1, n_x)
    xl = lax.rem(x + n_x - 1, n_x)
    xo = lax.rem(x + 2, n_x)

    home, away = c == 0, c == 1

    def dev(dd, xx, cc):
        return {'data': dd, 'model': xx * 2 + cc}

    def rc(src, dst, ss, rs, to):
        return pltpu.make_async_remote_copy(src_ref=src, dst_ref=dst, send_sem=ss, recv_sem=rs, device_id=to, device_id_type=MESH)

    other = dev(d, x, 1 - c)
    right = dev(d, xr, c)
    left = dev(d, xl, c)

    class Lay:
        pass

    lays = []
    for l in range(nl):
        L = Lay()
        L.l = l
        if l % 2 == 0:
            L.p, L.q, a = nbr1, nbr3, lax.div(d, 2)
        else:
            L.p, L.q, a = nbr3, nbr1, lax.rem(lax.div(d + 1, 2), 2)
        L.isb = (c - a) * (c - a)
        L.a_core, L.b_core = L.isb == 0, L.isb == 1
        L.src1 = L.p + (L.q - L.p) * L.isb
        L.srcx = L.q + (L.p - L.q) * L.isb
        L.src2 = opp + (d - opp) * L.isb
        L.first = dev(L.src1, x, c + (1 - 2 * c) * L.isb)
        L.pair = dev(L.p, x, c)
        lays.append(L)

    barrier = pltpu.get_barrier_semaphore()
    friends = [other, right, left, dev(nbr1, x, 0), dev(nbr1, x, 1), dev(nbr3, x, 0), dev(nbr3, x, 1), dev(opp, x, c)]
    for f in friends:
        pl.semaphore_signal(barrier, inc=1, device_id=f, device_id_type=MESH)
    xload = pltpu.make_async_copy(x_ref, xv, misc.at[0])
    xload.start()
    pl.semaphore_wait(barrier, len(friends))

    def cols(start, width):
        return pl.ds(start if isinstance(start, int) else pl.multiple_of(start, 128), width)

    class Unit:
        def __init__(self, L, s, parts_):
            self.L, self.idx, self.parts = L, (L.l * n_u + s) * 2, parts_

    def unit_in(L, s):
        l = L.l
        nz = min(s, 1) if isinstance(s, int) else lax.div(s + n_u - 1, n_u)
        starts = [hw + hw * s, (ff0 + ff + hw * (s - 2)) * nz]

        def part(c0):
            return (wi_ref.at[l, :, cols(c0, hw)], lambda e: wi_buf.at[l, e, :, cols(c0, hw)])
        u = Unit(L, s, [part(c0) for c0 in starts])
        u.s = s
        return u

    def each(u, fn):
        for i, (own, buf) in enumerate(u.parts):
            s = getattr(u, 's', 0)
            if i == 0 or (isinstance(s, int) and s != 1):
                fn(i, own, buf)
            elif not isinstance(s, int):
                @pl.when(s != 1)
                def _():
                    fn(i, own, buf)

    def unit_out(L, v):
        l = L.l
        cc = cols(v * cw, cw)
        return Unit(L, n_in + v, [(wa_ref.at[l, :, cc], lambda e: wa_buf.at[l, e, :, cc]), (wm_ref.at[l, :, cc], lambda e: wm_buf.at[l, e, :, cc])])

    def send_own(u, cond=None):
        L = u.L

        def go(i, own, buf):
            rc(own, buf(d), w_s1.at[u.idx + i], w_r1.at[u.idx + i], L.first).start()

        def go2(i, own, buf):
            rc(own, buf(d), w_s3.at[u.idx + i], w_d2.at[u.idx + i], other).start()

        if cond is None:
            each(u, go)
        else:
            @pl.when(L.a_core if cond == 'a' else L.b_core)
            def _():
                each(u, go)
        if cond != 'b':
            @pl.when(L.a_core)
            def _():
                each(u, go2)

    def fwd1(u, cond=None):
        L = u.L

        def go(i, own, buf):
            rc(own, buf(L.src1), w_s1.at[u.idx + i], w_r1.at[u.idx + i], L.first).wait_recv()

            @pl.when(L.b_core)
            def _():
                rc(buf(L.src1), buf(L.src1), w_s4.at[u.idx + i], w_r2.at[u.idx + i], L.pair).start()
            rc(buf(L.src1), buf(L.src1), w_s2.at[u.idx + i], w_d1.at[u.idx + i], other).start()

        if cond is None:
            each(u, go)
        else:
            @pl.when(L.a_core if cond == 'a' else L.b_core)
            def _():
                each(u, go)

    def fwd2(u):
        L = u.L

        def go(i, own, buf):
            rc(own, buf(opp), w_s4.at[u.idx + i], w_r2.at[u.idx + i], L.pair).wait_recv()
            rc(buf(opp), buf(opp), w_s3.at[u.idx + i], w_d2.at[u.idx + i], other).start()

        @pl.when(L.b_core)
        def _():
            each(u, go)

    def got1(u):
        each(u, lambda i, own, buf: rc(own, buf(u.L.srcx), w_s2.at[u.idx + i], w_d1.at[u.idx + i], other).wait_recv())

    def got2(u):
        each(u, lambda i, own, buf: rc(own, buf(u.L.src2), w_s3.at[u.idx + i], w_d2.at[u.idx + i], other).wait_recv())

    def sends_done(u):
        L = u.L

        def go(i, own, buf):
            rc(own, buf(d), w_s1.at[u.idx + i], w_r1.at[u.idx + i], L.first).wait_send()
            rc(own, buf(d), w_s2.at[u.idx + i], w_d1.at[u.idx + i], other).wait_send()
            rc(own, buf(d), w_s3.at[u.idx + i], w_d2.at[u.idx + i], other).wait_send()

            @pl.when(L.b_core)
            def _():
                rc(own, buf(d), w_s4.at[u.idx + i], w_r2.at[u.idx + i], L.pair).wait_send()
        each(u, go)

    def load_in(u, slot):
        L = u.L

        def go(i, own, buf):
            def to(e):
                return wv.at[slot, pl.ds(pl.multiple_of(e * dloc, dloc), dloc), pl.ds(i * hw, hw)]

            for e in (L.p, L.q, opp):
                pltpu.make_async_copy(buf(e), to(e), wld.at[slot]).start()

            @pl.when(L.a_core)
            def _():
                pltpu.make_async_copy(own, to(d), wld.at[slot]).start()

            @pl.when(L.b_core)
            def _():
                pltpu.make_async_copy(buf(d), to(d), wld.at[slot]).start()
        each(u, go)

    def wait_in(slot, w):
        pltpu.make_async_copy(wv.at[slot, :, pl.ds(0, w)], wv.at[slot, :, pl.ds(0, w)], wld.at[slot]).wait()

    def z_src(L, t):
        n2 = 2 * n_out
        late, r = lax.div(t, n2), lax.rem(t, n2)
        if L.l == 0:
            k = (1 - late) * lax.div(r, n_out) + late * (2 + lax.rem(r, 2))
            v = (1 - late) * lax.rem(r, n_out) + late * lax.div(r, 2)
        else:
            k, v = late + 2 * lax.rem(lax.div(t, n_out), 2), lax.rem(t, n_out)
        src = jnp.where(k == 0, d, jnp.where(k == 1, L.q, jnp.where(k == 2, L.p, opp)))
        return k, v, src

    def z_col(L, t):
        _, v, src = z_src(L, t)
        return src * n_out + v

    def load_out(L, t, wref, wsem):
        k, v, src = z_src(L, t)
        u = unit_out(L, v)
        spots = (wref.at[pl.ds(0, qw), :], wref.at[pl.ds(qw, ff), :])
        mine = jnp.logical_and(k == 0, L.a_core)

        @pl.when(mine)
        def _():
            for (own, buf), to in zip(u.parts, spots):
                pltpu.make_async_copy(own, to, wsem).start()

        @pl.when(jnp.logical_not(mine))
        def _():
            for (own, buf), to in zip(u.parts, spots):
                pltpu.make_async_copy(buf(src), to, wsem).start()

    def wait_out(wref, wsem):
        ref = wref.at[pl.ds(0, rw), :]
        pltpu.make_async_copy(ref, ref, wsem).wait()

    def wslot_of(slot):
        return wv.at[slot], wld.at[slot]

    def out_arrives(L, t):
        k, v, src = z_src(L, t)
        u = unit_out(L, v)

        @pl.when(jnp.logical_and(k == 0, L.b_core))
        def _():
            got2(u)

        @pl.when(jnp.logical_and(k == 1, L.a_core))
        def _():
            got1(u)

        if L.l == 0:
            @pl.when(jnp.logical_and(k == 2, L.a_core))
            def _():
                fwd1(u)

        @pl.when(jnp.logical_and(k == 2, L.b_core))
        def _():
            got1(u)

        if L.l == 0:
            @pl.when(k == 3)
            def _():
                fwd2(u)

        @pl.when(jnp.logical_and(k == 3, L.a_core))
        def _():
            got2(u)

    rows = 32

    def layer_norm(L, b):
        g = gfull[L.l:L.l + 1, :]

        def tile(i, _):
            r = pl.ds(pl.multiple_of(i * rows, rows), rows)
            v = xv[b, r, :].astype(F32)
            cen = v - jnp.mean(v, axis=-1, keepdims=True)
            var = jnp.mean(cen * cen, axis=-1, keepdims=True)
            h = (cen * lax.rsqrt(var + EPSILON) * g).astype(BF)
            hs[b, r, :] = h

            @pl.when(home)
            def _():
                hv[b, pl.ds(pl.multiple_of(m * sl + i * rows, rows), rows), :] = h
            return 0

        lax.fori_loop(0, sl // rows, tile, 0)

    def my_rows(b):
        return hv.at[b, pl.ds(pl.multiple_of(m * sl, sl), sl), :]

    def block(b, xx, lo=0, n=None):
        return hv.at[b, pl.ds(pl.multiple_of(xx * blk, blk), blk), pl.ds(lo, dm if n is None else n)]

    def ax(L, b):
        i = L.l * nb + b
        return rc(hs.at[b], my_rows(b), ax_s.at[i], ax_r.at[2 * i + c], dev(L.q, x, 1))

    def ad(L, b):
        i = L.l * nb + b
        return rc(hs.at[b], my_rows(b), ad_s.at[i], ad_r.at[i], other)

    def share(L, b):
        ax(L, b).start()

        @pl.when(away)
        def _():
            ad(L, b).start()

    def ring(L, b, way):
        i = 2 * (L.l * nb + b) + way
        return rc(block(b, x), block(b, x), rg_s.at[i], rg_r.at[i], right if way == 0 else left)

    def ring_in(L, b, way):
        i = 2 * (L.l * nb + b) + way
        src = block(b, xl if way == 0 else xr)
        return rc(src, src, rg_s.at[i], rg_r.at[i], right if way == 0 else left)

    def ring2(L, b, way, xx):
        i = 2 * (L.l * nb + b) + way
        src = block(b, xx, 0 if way == 0 else dm // 2, dm // 2)
        return rc(src, src, rf_s.at[i], rf_r.at[i], right if way == 0 else left)

    def ring_start(L, b):
        i = L.l * nb + b

        @pl.when(home)
        def _():
            dst = hv.at[b, pl.ds(pl.multiple_of(x * blk + sl, sl), sl), :]
            rc(hs.at[b], dst, ad_s.at[i], ad_r.at[i], other).wait_recv()

        @pl.when(away)
        def _():
            for cc in range(2):
                dst = hv.at[b, pl.ds(pl.multiple_of(x * blk + cc * sl, sl), sl), :]
                rc(hs.at[b], dst, ax_s.at[i], ax_r.at[2 * i + cc], other).wait_recv()
        for way in range(2):
            ring(L, b, way).start()

    def ring_pass(L, b):
        for way in range(2):
            ring_in(L, b, way).wait_recv()
            ring2(L, b, way, xl if way == 0 else xr).start()

    def ring_end(L, b):
        for way in range(2):
            ring2(L, b, way, xo).wait_recv()

    def gather_sends_done(L, b):
        ax(L, b).wait_send()

        @pl.when(away)
        def _():
            ad(L, b).wait_send()
        for way in range(2):
            ring(L, b, way).wait_send()
            ring2(L, b, way, xl if way == 0 else xr).wait_send()

    def p_qkv(b):
        def step(i, _):
            col = hw * (1 - i) + 3 * hw * lax.div(i, 2)
            w = wv[lax.div(i, 2), :, cols(lax.rem(i, 2) * hw, hw)]
            qkv[b, :, cols(col, hw)] = jnp.dot(hv[b], w, preferred_element_type=F32).astype(BF)
            return 0
        lax.fori_loop(0, 3, step, 0)

    def p_gu(b, slot, k):
        acc = jnp.dot(hv[b], wv[slot], preferred_element_type=F32)
        g = acc[:, 0:hw].astype(BF).astype(F32)
        up = acc[:, hw:cw].astype(BF).astype(F32)
        om[b, :, cols(qw + hw * k, hw)] = (g * (1.0 / (1.0 + jnp.exp(-g))) * up).astype(BF)

    def attention(b):
        tq = 256
        kl = kcur[b, 0:1, 0:1]
        for i in range(seq // tq):
            n = tq * (i + 1)
            row = lax.broadcasted_iota(jnp.int32, (tq, n), 0) + tq * i
            col = lax.broadcasted_iota(jnp.int32, (tq, n), 1)
            ok = jnp.logical_and(col <= row, col < kl)

            def head(h, _):
                hc = pl.ds(pl.multiple_of(h * hd, hd), hd)
                qh = qkv[b, tq * i:tq * (i + 1), hc]
                s = lax.dot_general(qh, qkv[b, 0:n, kv0:kv0 + hd], (((1,), (1,)), ((), ())), preferred_element_type=F32) * hd ** -0.5
                s = jnp.where(ok, s, NEG_BIG)
                e = jnp.exp(s - jnp.max(s, axis=-1, keepdims=True))
                tot = jnp.sum(e, axis=-1, keepdims=True)
                o = jnp.dot(e.astype(BF), qkv[b, 0:n, kv0 + hd:kv0 + 2 * hd], preferred_element_type=F32)
                om[b, tq * i:tq * (i + 1), hc] = (o / tot).astype(BF)
                return 0

            lax.fori_loop(0, qw // hd, head, 0)

    def zblk(slot, xx, lo, n):
        return zs.at[slot, pl.ds(pl.multiple_of(xx * blk, blk), blk), pl.ds(lo, n)]

    def a_send(slot, way):
        return rc(zblk(slot, xo, way * hw, hw), ra.at[slot, way], a_s.at[2 * slot + way], a_r.at[2 * slot + way], right if way == 0 else left)

    def b_send(slot, way):
        return rc(zblk(slot, xr if way == 0 else xl, 0, cw), rb.at[slot, way], b_s.at[2 * slot + way], b_r.at[2 * slot + way],
                  right if way == 0 else left)

    def z_step(b, wref, j):
        slot = lax.rem(j, NS)

        @pl.when(j >= NS)
        def _():
            for way in range(2):
                a_send(slot, way).wait_send()
                b_send(slot, way).wait_send()
        zs[slot] = jnp.dot(om[b], wref[0:rw, :], preferred_element_type=F32).astype(BF)
        for way in range(2):
            a_send(slot, way).start()

    def rs_b(j):
        slot = lax.rem(j, NS)
        for way in range(2):
            a_send(slot, way).wait_recv()
            r = pl.ds(pl.multiple_of((xr if way == 0 else xl) * blk, blk), blk)
            cc = pl.ds(way * hw, hw)
            zs[slot, r, cc] = (zs[slot, r, cc].astype(F32) + ra[slot, way].astype(F32)).astype(BF)
        for way in range(2):
            b_send(slot, way).start()

    def c_send(L, b, n, slot, cc, inside):
        i = (L.l * n_t + n) * nb + b
        sem = c_s.at[2 * slot + cc]
        if inside:
            return rc(cst.at[slot, pl.ds(cc * sl, sl), :], parts.at[0, b, :, cols(n * cw, cw)], sem, pd_r.at[i], other)
        return rc(cst.at[slot, pl.ds(cc * sl, sl), :], parts.at[1, b, :, cols(n * cw, cw)], sem, pa_r.at[i], dev(L.q, x, cc))

    def c_wait(L, slot):
        @pl.when(away)
        def _():
            for cc in range(2):
                c_send(L, 0, 0, slot, cc, False).wait_send()

        @pl.when(home)
        def _():
            c_send(L, 0, 0, slot, 1, True).wait_send()

    def rs_c(L, j, b, t):
        slot, cslot = lax.rem(j, NS), lax.rem(j, NC)
        n = z_col(L, t)
        for way in range(2):
            b_send(slot, way).wait_recv()

        @pl.when(j >= NC)
        def _():
            c_wait(L, cslot)
        r = pl.ds(pl.multiple_of(x * blk, blk), blk)
        cst[cslot] = (zs[slot, r, :].astype(F32) + rb[slot, 0].astype(F32) + rb[slot, 1].astype(F32)).astype(BF)

        @pl.when(home)
        def _():
            c_send(L, b, n, cslot, 1, True).start()
            parts[0, b, :, cols(n * cw, cw)] = cst[cslot, 0:sl, :]

        @pl.when(away)
        def _():
            for cc in range(2):
                c_send(L, b, n, cslot, cc, False).start()

    def combine(L, b):
        for n in range(n_t):
            c_send(L, b, n, 0, 0, False).wait_recv()

            @pl.when(away)
            def _():
                c_send(L, b, n, 0, 0, True).wait_recv()

        def tile(i, _):
            r = pl.ds(pl.multiple_of(i * rows, rows), rows)
            z = parts[0, b, r, :].astype(F32) + parts[1, b, r, :].astype(F32)
            xv[b, r, :] = (xv[b, r, :].astype(F32) + z).astype(BF)
            return 0

        lax.fori_loop(0, sl // rows, tile, 0)

    L0, L1 = lays
    g_to = [dev(nbr1, x, c), dev(nbr3, x, c), dev(opp, x, c)]

    def gsl(e):
        return gfull.at[:, pl.ds(pl.multiple_of(e * dloc, dloc), dloc)]

    for i in range(3):
        rc(gain_ref, gsl(d), g_s.at[i], g_r.at[i], g_to[i]).start()

    @pl.when(away)
    def _():
        for l, L in enumerate(lays):
            rc(kl_ref, klb.at[l], k_s.at[l], k_r.at[l], dev(L.q, x, 1)).start()
    gfull[:, pl.ds(pl.multiple_of(d * dloc, dloc), dloc)] = gain_ref[...]

    def set_len(L):
        @pl.when(home)
        def _():
            kcur[...] = kl_ref[...]

        @pl.when(away)
        def _():
            rc(kl_ref, klb.at[L.l], k_s.at[L.l], k_r.at[L.l], other).wait_recv()
            kcur[...] = klb[L.l]

    def loop(n, fn, start=0):
        def body(i, _):
            fn(i)
            return 0
        lax.fori_loop(start, n, body, 0)

    def both(*conds):
        r = conds[0]
        for q in conds[1:]:
            r = jnp.logical_and(r, q)
        return r

    xload.wait()
    for i, e in enumerate((nbr1, nbr3, opp)):
        rc(gain_ref, gsl(e), g_s.at[i], g_r.at[i], g_to[i]).wait_recv()
    loop(n_in, lambda s: send_own(unit_in(L0, s), 'a'))
    layer_norm(L0, 0)
    share(L0, 0)
    layer_norm(L0, 1)
    loop(2, lambda s: send_own(unit_in(L0, s), 'b'))
    share(L0, 1)
    loop(n_in, lambda s: send_own(unit_in(L0, s), 'b'), 2)
    loop(n_out, lambda v: send_own(unit_out(L0, v), 'b'))
    set_len(L0)

    def in_ready(L, s):
        u = unit_in(L, s)
        fwd2(u)
        got1(u)
        got2(u)

    def fa(L, s):
        fwd1(unit_in(L, s), 'a')

    def fb(L, s):
        fwd1(unit_in(L, s), 'b')

    ring_start(L0, 0)
    for s in range(3):
        fa(L0, s)

    @pl.when(home)
    def _():
        ring_pass(L0, 0)
    fb(L0, 0)
    fb(L0, 1)
    fa(L0, 3)

    @pl.when(away)
    def _():
        ring_pass(L0, 0)
    fa(L0, 4)
    ring_start(L0, 1)
    fwd2(unit_in(L0, 0))
    fa(L0, 5)
    fb(L0, 2)
    fwd2(unit_in(L0, 1))
    ring_end(L0, 0)
    n_early = 2

    def stage0(b):
        first = b == 0

        @pl.when(first)
        def _():
            for s in range(2):
                got1(unit_in(L0, s))
                got2(unit_in(L0, s))

        @pl.when(jnp.logical_not(first))
        def _():
            fb(L0, 7)
            ring_end(L0, 1)
        load_in(unit_in(L0, 0), 0)
        load_in(unit_in(L0, 1), 1)
        wait_in(0, cw)
        wait_in(1, hw)
        p_qkv(b)

        @pl.when(first)
        def _():
            fb(L0, 3)
        attention(b)

        @pl.when(first)
        def _():
            fb(L0, 4)
            fa(L0, 6)
            in_ready(L0, 2)

        @pl.when(jnp.logical_not(first))
        def _():
            fb(L0, 8)
            fa(L0, 8)
        load_in(unit_in(L0, 2), 0)

        def gu(k):
            slot = lax.rem(k, 2)
            wait_in(slot, cw)
            p_gu(b, slot, k)

            @pl.when(both(first, k == 0))
            def _():
                fb(L0, 5)
                ring_pass(L0, 1)
                fb(L0, 6)
                fa(L0, 7)
                in_ready(L0, 3)

            @pl.when(both(jnp.logical_not(first), k == 0))
            def _():
                fwd2(unit_in(L0, 4))

            @pl.when(k + 1 < n_early)
            def _():
                load_in(unit_in(L0, k + 3), 1 - slot)
        loop(n_early, gu)

    loop(nb, stage0)
    fb(L0, 9)
    u4 = unit_in(L0, n_early + 2)
    got1(u4)
    got2(u4)
    load_in(u4, n_early % 2)

    def gu0(k):
        s = k + 2
        slot = lax.rem(k, 2)
        wait_in(slot, cw)
        p_gu(0, slot, k)

        @pl.when(k == n_early)
        def _():
            fa(L0, 9)

        @pl.when(both(k >= n_gu - 1 - n_out, k < n_gu - 1))
        def _():
            fwd1(unit_out(L0, k - (n_gu - 1 - n_out)), 'b')

        @pl.when(k == n_gu // 2)
        def _():
            loop(n_out, lambda v: send_own(unit_out(L0, v), 'a'))

        @pl.when(s + 1 < n_in)
        def _():
            in_ready(L0, s + 1)
            load_in(unit_in(L0, s + 1), 1 - slot)

        @pl.when(s + 1 == n_in)
        def _():
            out_arrives(L0, 0)
            load_out(L0, 0, *wslot_of(1 - slot))
        p_gu(1, slot, k)

        @pl.when(both(k >= n_gu - 4, k < n_gu - 2))
        def _():
            for i in range(2):
                send_own(unit_in(L1, 2 * (k - (n_gu - 4)) + i), 'a')

        @pl.when(k >= n_gu - 2)
        def _():
            send_own(unit_in(L1, k - (n_gu - 2) + 4), 'a')

    loop(n_gu, gu0, n_early)
    for b in range(nb):
        gather_sends_done(L0, b)

    @pl.when(away)
    def _():
        for cc in range(2):
            pl.semaphore_signal(free_sem, inc=1, device_id=dev(L1.q, x, cc), device_id_type=MESH)
    z0 = n_gu % 2
    j_end = nb * n_t
    j_late = j_end // 2

    assert nb == 2 and n_t == 8

    def pick(i, values):
        r = values[-1]
        for k in range(len(values) - 1):
            r = jnp.where(i == k, values[k], r)
        return r

    def jt(j):
        late, r = lax.div(j, j_late), lax.rem(j, j_late)
        b = (1 - late) * lax.rem(r, nb) + late * pick(r, (0, 0, 1, 0, 0, 1, 1, 1))
        t = (1 - late) * lax.div(r, nb) + late * (n_t // 2 + pick(r, (0, 1, 0, 2, 3, 1, 2, 3)))
        return b, t

    def z_loop0(j):
        slot = lax.rem(j + z0, 2)
        b, t = jt(j)
        wait_out(*wslot_of(slot))
        z_step(b, wv.at[slot], j)

        @pl.when(j + 1 < j_end)
        def _():
            b1, t1 = jt(j + 1)

            @pl.when(b1 == 0)
            def _():
                out_arrives(L0, t1)
            load_out(L0, t1, *wslot_of(1 - slot))

        @pl.when(j >= 1)
        def _():
            rs_b(j - 1)

        @pl.when(j >= 2)
        def _():
            b2, t2 = jt(j - 2)
            rs_c(L0, j - 2, b2, t2)
        half = lax.div(j, 2)

        @pl.when(both(lax.rem(j, 2) == 1, half + 6 < n_in))
        def _():
            send_own(unit_in(L1, half + 6), 'a')

        @pl.when(lax.rem(j, 2) == 1)
        def _():
            fa(L1, half)

        @pl.when(j == j_late)
        def _():
            send_own(unit_out(L1, 0), 'a')

        @pl.when(both(j >= j_end - 5, lax.rem(j, 2) == 1, j < j_end - 1))
        def _():
            for i in range(2):
                send_own(unit_in(L1, j - (j_end - 5) + i), 'b')

    loop(j_end, z_loop0)
    pl.semaphore_wait(free_sem, 1)
    combine(L0, 0)
    layer_norm(L1, 0)
    share(L1, 0)
    rs_b(j_end - 1)
    rs_c(L0, j_end - 2, nb - 1, n_t - 2)
    rs_c(L0, j_end - 1, nb - 1, n_t - 1)

    @pl.when(home)
    def _():
        ring_start(L1, 0)
    for s in range(3):
        fb(L1, s)
    combine(L0, 1)
    layer_norm(L1, 1)
    share(L1, 1)
    send_own(unit_in(L1, 4), 'b')
    loop(n_in, lambda s: send_own(unit_in(L1, s), 'b'), 5)
    loop(n_out, lambda v: send_own(unit_out(L1, v), 'b'))
    loop(n_in, lambda s: fa(L1, s), n_in - 2)
    set_len(L1)

    @pl.when(away)
    def _():
        ring_start(L1, 0)
    fb(L1, 3)
    in_ready(L1, 0)
    load_in(unit_in(L1, 0), 0)
    in_ready(L1, 1)
    load_in(unit_in(L1, 1), 1)

    @pl.when(home)
    def _():
        ring_pass(L1, 0)
    fwd2(unit_in(L1, 2))
    send_own(unit_out(L1, 1), 'a')
    fb(L1, 4)

    @pl.when(away)
    def _():
        ring_pass(L1, 0)
        ring_start(L1, 1)
    fb(L1, 5)
    fwd2(unit_in(L1, 3))
    fb(L1, 6)
    fwd2(unit_in(L1, 4))
    assert n_gu == n_t

    def stage1(b):
        first = b == 0

        @pl.when(jnp.logical_not(first))
        def _():
            load_in(unit_in(L1, 0), 0)
            load_in(unit_in(L1, 1), 1)
        ring_end(L1, b)
        wait_in(0, cw)
        wait_in(1, hw)
        p_qkv(b)

        @pl.when(first)
        def _():
            fb(L1, 7)
            fwd2(unit_in(L1, 5))
            got1(unit_in(L1, 2))
            got2(unit_in(L1, 2))

        @pl.when(both(first, home))
        def _():
            ring_start(L1, 1)
        load_in(unit_in(L1, 2), 0)

        @pl.when(jnp.logical_not(first))
        def _():
            fwd1(unit_out(L1, 1), 'b')
            out_arrives(L1, 0)
            load_out(L1, 0, wz, wzs.at[0])
        attention(b)

        @pl.when(first)
        def _():
            fb(L1, 8)
            fwd2(unit_in(L1, 6))

        def gu(k):
            slot = lax.rem(k, 2)

            @pl.when(both(first, k == 0))
            def _():
                fb(L1, n_in - 1)

            @pl.when(both(first, k + 7 < n_in))
            def _():
                fwd2(unit_in(L1, k + 7))

            @pl.when(both(first, k >= n_gu - n_out))
            def _():
                fwd1(unit_out(L1, k - (n_gu - n_out)), 'a')

            @pl.when(both(first, k == n_gu - 2))
            def _():
                fwd1(unit_out(L1, 0), 'b')

            @pl.when(both(jnp.logical_not(first), k >= 3, k < 3 + n_out))
            def _():
                fwd2(unit_out(L1, k - 3))

            @pl.when(both(first, k + 1 < n_gu))
            def _():
                got1(unit_in(L1, k + 3))
                got2(unit_in(L1, k + 3))

            @pl.when(k + 1 < n_gu)
            def _():
                load_in(unit_in(L1, k + 3), 1 - slot)
            wait_in(slot, cw)
            p_gu(b, slot, k)

            @pl.when(both(first, k == 5))
            def _():
                ring_pass(L1, 1)

            @pl.when(jnp.logical_not(first))
            def _():
                wait_out(wz, wzs.at[0])
                j = j_end + k
                z_step(0, wz, j)

                @pl.when(k >= 1)
                def _():
                    rs_b(j - 1)

                @pl.when(k >= 2)
                def _():
                    rs_c(L1, j - 2, 0, k - 2)

                @pl.when(k + 1 < n_t)
                def _():
                    out_arrives(L1, k + 1)
                    load_out(L1, k + 1, wz, wzs.at[0])
        loop(n_gu, gu)

    loop(nb, stage1)
    load_out(L1, 0, *wslot_of(0))
    for b in range(nb):
        gather_sends_done(L1, b)

    def z_loop1(t):
        wslot = lax.rem(t, 2)
        wait_out(*wslot_of(wslot))

        @pl.when(t + 1 < n_t)
        def _():
            load_out(L1, t + 1, *wslot_of(1 - wslot))
        j = j_end + n_t + t
        z_step(1, wv.at[wslot], j)
        rs_b(j - 1)
        i2 = n_t + t - 2
        rs_c(L1, j - 2, lax.div(i2, n_t), lax.rem(i2, n_t))

    loop(n_t, z_loop1)
    j_last = 2 * j_end - 1
    rs_b(j_last)
    rs_c(L1, j_last - 1, 1, n_t - 2)
    rs_c(L1, j_last, 1, n_t - 1)
    for b in range(nb):
        combine(L1, b)
    yout = pltpu.make_async_copy(xv, y_ref, misc.at[0])
    yout.start()

    def layer_sends_done(L):
        loop(n_in, lambda s: sends_done(unit_in(L, s)))
        loop(n_out, lambda v: sends_done(unit_out(L, v)))

    layer_sends_done(L0)
    layer_sends_done(L1)
    for i in range(3):
        rc(gain_ref, gsl(d), g_s.at[i], g_r.at[i], g_to[i]).wait_send()

    @pl.when(away)
    def _():
        for l in range(nl):
            rc(kl_ref, klb.at[l], k_s.at[l], k_r.at[l], other).wait_send()
    for slot in range(NC):
        c_wait(L1, slot)
    for slot in range(NS):
        for way in range(2):
            a_send(slot, way).wait_send()
            b_send(slot, way).wait_send()
    yout.wait()


def solution(mesh):
    n_data = mesh.shape['data']
    n_x = mesh.shape['model'] // 2
    batch_axes = ('rep', 'data')

    def device_step(x_loc, len_loc, gain_loc, w_in_loc, w_attn_loc, w_mlp_loc):
        nl, dloc, block_in = w_in_loc.shape
        qw, ff = w_attn_loc.shape[1], w_mlp_loc.shape[1]
        hd = (block_in - qw - 2 * ff) // 2
        nb, sl, dm = x_loc.shape
        seq = sl * 2 * n_x
        cfg = (n_data, n_x, nb, sl, dm, dloc, qw, hd, ff, nl)
        cw = 512
        n_u = 2 + ff // (cw // 2) + dloc // cw
        n_t = n_data * (dloc // cw)
        lens = jnp.broadcast_to(len_loc[:, None, None], (nb, 8, 128))
        gain = gain_loc.astype(F32)
        anyspec = pl.BlockSpec(memory_space=pl.ANY)
        vspec = pl.BlockSpec(memory_space=pltpu.VMEM)
        sem = pltpu.SemaphoreType.DMA
        out = pl.pallas_call(
            functools.partial(kernel, cfg),
            out_shape=[
                jax.ShapeDtypeStruct((nb, sl, dm), BF),
                jax.ShapeDtypeStruct((nl, n_data, dloc, block_in), BF),
                jax.ShapeDtypeStruct((nl, n_data, qw, dloc), BF),
                jax.ShapeDtypeStruct((nl, n_data, ff, dloc), BF),
            ],
            in_specs=[anyspec, vspec, vspec, anyspec, anyspec, anyspec],
            out_specs=[anyspec] * 4,
            scratch_shapes=[
                pltpu.VMEM((nb, seq, dm), BF),
                pltpu.VMEM((nb, seq, qw + 2 * hd), BF),
                pltpu.VMEM((nb, seq, qw + ff), BF),
                pltpu.VMEM((2, dm, cw), BF),
                pltpu.VMEM((qw + ff, cw), BF),
                pltpu.VMEM((NS, seq, cw), BF),
                pltpu.VMEM((NS, 2, 2 * sl, cw // 2), BF),
                pltpu.VMEM((NS, 2, 2 * sl, cw), BF),
                pltpu.VMEM((NC, 2 * sl, cw), BF),
                pltpu.VMEM((2, nb, sl, dm), BF),
                pltpu.VMEM((nb, sl, dm), BF),
                pltpu.VMEM((nb, sl, dm), BF),
                pltpu.VMEM((nl, dm), F32),
                pltpu.VMEM((nl, nb, 8, 128), jnp.int32),
                pltpu.VMEM((nb, 8, 128), jnp.int32),
            ] + [sem((nl * n_u * 2,))] * 8 + [
                sem((2,)),
                sem((1,)),
                sem((1,)),
                sem((3,)), sem((3,)),
                sem((nl,)), sem((nl,)),
                sem((nl * nb,)), sem((nl * nb * 2,)),
                sem((nl * nb,)), sem((nl * nb,)),
                sem((nl * nb * 2,)), sem((nl * nb * 2,)),
                sem((nl * nb * 2,)), sem((nl * nb * 2,)),
                sem((NS * 2,)), sem((NS * 2,)), sem((NS * 2,)), sem((NS * 2,)), sem((NC * 2,)),
                sem((nl * n_t * nb,)), sem((nl * n_t * nb,)),
                pltpu.SemaphoreType.REGULAR,
            ],
            compiler_params=pltpu.CompilerParams(collective_id=0, has_side_effects=True, vmem_limit_bytes=63 * 1024 * 1024),
        )(x_loc, lens, gain, w_in_loc, w_attn_loc, w_mlp_loc)
        return out[0]

    return jax.shard_map(device_step, mesh=mesh, in_specs=(P(batch_axes, 'model', None), P(batch_axes), P(None, 'data'), P(None, 'data', 'model'), P(None, 'model', 'data'), P(None, 'model', 'data')), out_specs=P(batch_axes, 'model', None), check_vma=False)
```

```python
import functools

import jax
import jax.numpy as jnp
from jax import lax
from jax.experimental import pallas as pl
from jax.experimental.pallas import tpu as pltpu
from jax.sharding import PartitionSpec as P

EPSILON = 1e-6
NEG_BIG = -1e30
MESH = pl.DeviceIdType.MESH
BF = jnp.bfloat16
F32 = jnp.float32
NS = 3
NC = 8


def kernel(cfg, x_ref, kl_ref, gain_ref, wi_ref, wa_ref, wm_ref,
           y_ref, wi_buf, wa_buf, wm_buf,
           hv, qkv, om, wv, wz, zs, ra, rb, cst, parts, xv, hs, gfull, klb, kcur,
           w_r1, w_r2, w_d1, w_d2, w_s1, w_s2, w_s3, w_s4, wld, wzs, misc,
           g_s, g_r, k_s, k_r, ax_s, ax_r, ad_s, ad_r, rg_s, rg_r, rf_s, rf_r,
           a_s, a_r, b_s, b_r, c_s, pd_r, pa_r, free_sem):
    (n_data, n_x, nb, sl, dm, dloc, qw, hd, ff, nl) = cfg
    seq = sl * 2 * n_x
    blk = 2 * sl
    cw = 512
    hw = cw // 2
    kv0 = qw
    ff0 = qw + 2 * hd
    n_gu = ff // hw
    n_in = 2 + n_gu
    n_out = dloc // cw
    n_u = n_in + n_out
    n_t = n_data * n_out
    rw = qw + ff

    d = lax.axis_index('data')
    m = lax.axis_index('model')
    x = lax.div(m, 2)
    c = lax.rem(m, 2)
    d_odd = lax.rem(d, 2)
    nbr1 = d + 1 - 2 * d_odd
    nbr3 = n_data - 1 - d
    opp = lax.rem(d + 2, n_data)
    xr = lax.rem(x + 1, n_x)
    xl = lax.rem(x + n_x - 1, n_x)
    xo = lax.rem(x + 2, n_x)

    home, away = c == 0, c == 1

    def dev(dd, xx, cc):
        return {'data': dd, 'model': xx * 2 + cc}

    def rc(src, dst, ss, rs, to):
        return pltpu.make_async_remote_copy(src_ref=src, dst_ref=dst, send_sem=ss, recv_sem=rs, device_id=to, device_id_type=MESH)

    other = dev(d, x, 1 - c)
    right = dev(d, xr, c)
    left = dev(d, xl, c)

    class Lay:
        pass

    lays = []
    for l in range(nl):
        L = Lay()
        L.l = l
        if l % 2 == 0:
            L.p, L.q, a = nbr1, nbr3, lax.div(d, 2)
        else:
            L.p, L.q, a = nbr3, nbr1, lax.rem(lax.div(d + 1, 2), 2)
        L.isb = (c - a) * (c - a)
        L.a_core, L.b_core = L.isb == 0, L.isb == 1
        L.src1 = L.p + (L.q - L.p) * L.isb
        L.srcx = L.q + (L.p - L.q) * L.isb
        L.src2 = opp + (d - opp) * L.isb
        L.first = dev(L.src1, x, c + (1 - 2 * c) * L.isb)
        L.pair = dev(L.p, x, c)
        lays.append(L)

    barrier = pltpu.get_barrier_semaphore()
    friends = [other, right, left, dev(nbr1, x, 0), dev(nbr1, x, 1), dev(nbr3, x, 0), dev(nbr3, x, 1), dev(opp, x, c)]
    for f in friends:
        pl.semaphore_signal(barrier, inc=1, device_id=f, device_id_type=MESH)
    xload = pltpu.make_async_copy(x_ref, xv, misc.at[0])
    xload.start()
    pl.semaphore_wait(barrier, len(friends))

    def cols(start, width):
        return pl.ds(start if isinstance(start, int) else pl.multiple_of(start, 128), width)

    class Unit:
        def __init__(self, L, s, parts_):
            self.L, self.idx, self.parts = L, (L.l * n_u + s) * 2, parts_

    def unit_in(L, s):
        l = L.l
        nz = min(s, 1) if isinstance(s, int) else lax.div(s + n_u - 1, n_u)
        starts = [hw + hw * s, (ff0 + ff + hw * (s - 2)) * nz]

        def part(c0):
            return (wi_ref.at[l, :, cols(c0, hw)], lambda e: wi_buf.at[l, e, :, cols(c0, hw)])
        u = Unit(L, s, [part(c0) for c0 in starts])
        u.s = s
        return u

    def each(u, fn):
        for i, (own, buf) in enumerate(u.parts):
            s = getattr(u, 's', 0)
            if i == 0 or (isinstance(s, int) and s != 1):
                fn(i, own, buf)
            elif not isinstance(s, int):
                @pl.when(s != 1)
                def _():
                    fn(i, own, buf)

    def unit_out(L, v):
        l = L.l
        cc = cols(v * cw, cw)
        return Unit(L, n_in + v, [(wa_ref.at[l, :, cc], lambda e: wa_buf.at[l, e, :, cc]), (wm_ref.at[l, :, cc], lambda e: wm_buf.at[l, e, :, cc])])

    def send_own(u, cond=None):
        L = u.L

        def go(i, own, buf):
            rc(own, buf(d), w_s1.at[u.idx + i], w_r1.at[u.idx + i], L.first).start()

        def go2(i, own, buf):
            rc(own, buf(d), w_s3.at[u.idx + i], w_d2.at[u.idx + i], other).start()

        if cond is None:
            each(u, go)
        else:
            @pl.when(L.a_core if cond == 'a' else L.b_core)
            def _():
                each(u, go)
        if cond != 'b':
            @pl.when(L.a_core)
            def _():
                each(u, go2)

    def fwd1(u, cond=None):
        L = u.L

        def go(i, own, buf):
            rc(own, buf(L.src1), w_s1.at[u.idx + i], w_r1.at[u.idx + i], L.first).wait_recv()

            @pl.when(L.b_core)
            def _():
                rc(buf(L.src1), buf(L.src1), w_s4.at[u.idx + i], w_r2.at[u.idx + i], L.pair).start()
            rc(buf(L.src1), buf(L.src1), w_s2.at[u.idx + i], w_d1.at[u.idx + i], other).start()

        if cond is None:
            each(u, go)
        else:
            @pl.when(L.a_core if cond == 'a' else L.b_core)
            def _():
                each(u, go)

    def fwd2(u):
        L = u.L

        def go(i, own, buf):
            rc(own, buf(opp), w_s4.at[u.idx + i], w_r2.at[u.idx + i], L.pair).wait_recv()
            rc(buf(opp), buf(opp), w_s3.at[u.idx + i], w_d2.at[u.idx + i], other).start()

        @pl.when(L.b_core)
        def _():
            each(u, go)

    def got1(u):
        each(u, lambda i, own, buf: rc(own, buf(u.L.srcx), w_s2.at[u.idx + i], w_d1.at[u.idx + i], other).wait_recv())

    def got2(u):
        each(u, lambda i, own, buf: rc(own, buf(u.L.src2), w_s3.at[u.idx + i], w_d2.at[u.idx + i], other).wait_recv())

    def sends_done(u):
        L = u.L

        def go(i, own, buf):
            rc(own, buf(d), w_s1.at[u.idx + i], w_r1.at[u.idx + i], L.first).wait_send()
            rc(own, buf(d), w_s2.at[u.idx + i], w_d1.at[u.idx + i], other).wait_send()
            rc(own, buf(d), w_s3.at[u.idx + i], w_d2.at[u.idx + i], other).wait_send()

            @pl.when(L.b_core)
            def _():
                rc(own, buf(d), w_s4.at[u.idx + i], w_r2.at[u.idx + i], L.pair).wait_send()
        each(u, go)

    def load_in(u, slot):
        L = u.L

        def go(i, own, buf):
            def to(e):
                return wv.at[slot, pl.ds(pl.multiple_of(e * dloc, dloc), dloc), pl.ds(i * hw, hw)]

            for e in (L.p, L.q, opp):
                pltpu.make_async_copy(buf(e), to(e), wld.at[slot]).start()

            @pl.when(L.a_core)
            def _():
                pltpu.make_async_copy(own, to(d), wld.at[slot]).start()

            @pl.when(L.b_core)
            def _():
                pltpu.make_async_copy(buf(d), to(d), wld.at[slot]).start()
        each(u, go)

    def wait_in(slot, w):
        pltpu.make_async_copy(wv.at[slot, :, pl.ds(0, w)], wv.at[slot, :, pl.ds(0, w)], wld.at[slot]).wait()

    def z_src(L, t):
        n2 = 2 * n_out
        late, r = lax.div(t, n2), lax.rem(t, n2)
        if L.l == 0:
            k = (1 - late) * lax.div(r, n_out) + late * (2 + lax.rem(r, 2))
            v = (1 - late) * lax.rem(r, n_out) + late * lax.div(r, 2)
        else:
            k, v = late + 2 * lax.rem(lax.div(t, n_out), 2), lax.rem(t, n_out)
        src = jnp.where(k == 0, d, jnp.where(k == 1, L.q, jnp.where(k == 2, L.p, opp)))
        return k, v, src

    def z_col(L, t):
        _, v, src = z_src(L, t)
        return src * n_out + v

    def load_out(L, t, wref, wsem):
        k, v, src = z_src(L, t)
        u = unit_out(L, v)
        spots = (wref.at[pl.ds(0, qw), :], wref.at[pl.ds(qw, ff), :])
        mine = jnp.logical_and(k == 0, L.a_core)

        @pl.when(mine)
        def _():
            for (own, buf), to in zip(u.parts, spots):
                pltpu.make_async_copy(own, to, wsem).start()

        @pl.when(jnp.logical_not(mine))
        def _():
            for (own, buf), to in zip(u.parts, spots):
                pltpu.make_async_copy(buf(src), to, wsem).start()

    def wait_out(wref, wsem):
        ref = wref.at[pl.ds(0, rw), :]
        pltpu.make_async_copy(ref, ref, wsem).wait()

    def wslot_of(slot):
        return wv.at[slot], wld.at[slot]

    def out_arrives(L, t):
        k, v, src = z_src(L, t)
        u = unit_out(L, v)

        @pl.when(jnp.logical_and(k == 0, L.b_core))
        def _():
            got2(u)

        @pl.when(jnp.logical_and(k == 1, L.a_core))
        def _():
            got1(u)

        if L.l == 0:
            @pl.when(jnp.logical_and(k == 2, L.a_core))
            def _():
                fwd1(u)

        @pl.when(jnp.logical_and(k == 2, L.b_core))
        def _():
            got1(u)

        if L.l == 0:
            @pl.when(k == 3)
            def _():
                fwd2(u)

        @pl.when(jnp.logical_and(k == 3, L.a_core))
        def _():
            got2(u)

    rows = 32

    def layer_norm(L, b):
        g = gfull[L.l:L.l + 1, :]

        def tile(i, _):
            r = pl.ds(pl.multiple_of(i * rows, rows), rows)
            v = xv[b, r, :].astype(F32)
            cen = v - jnp.mean(v, axis=-1, keepdims=True)
            var = jnp.mean(cen * cen, axis=-1, keepdims=True)
            h = (cen * lax.rsqrt(var + EPSILON) * g).astype(BF)
            hs[b, r, :] = h

            @pl.when(home)
            def _():
                hv[b, pl.ds(pl.multiple_of(m * sl + i * rows, rows), rows), :] = h
            return 0

        lax.fori_loop(0, sl // rows, tile, 0)

    def my_rows(b):
        return hv.at[b, pl.ds(pl.multiple_of(m * sl, sl), sl), :]

    def block(b, xx, lo=0, n=None):
        return hv.at[b, pl.ds(pl.multiple_of(xx * blk, blk), blk), pl.ds(lo, dm if n is None else n)]

    def ax(L, b):
        i = L.l * nb + b
        return rc(hs.at[b], my_rows(b), ax_s.at[i], ax_r.at[2 * i + c], dev(L.q, x, 1))

    def ad(L, b):
        i = L.l * nb + b
        return rc(hs.at[b], my_rows(b), ad_s.at[i], ad_r.at[i], other)

    def share(L, b):
        ax(L, b).start()

        @pl.when(away)
        def _():
            ad(L, b).start()

    def ring(L, b, way):
        i = 2 * (L.l * nb + b) + way
        return rc(block(b, x), block(b, x), rg_s.at[i], rg_r.at[i], right if way == 0 else left)

    def ring_in(L, b, way):
        i = 2 * (L.l * nb + b) + way
        src = block(b, xl if way == 0 else xr)
        return rc(src, src, rg_s.at[i], rg_r.at[i], right if way == 0 else left)

    def ring2(L, b, way, xx):
        i = 2 * (L.l * nb + b) + way
        src = block(b, xx, 0 if way == 0 else dm // 2, dm // 2)
        return rc(src, src, rf_s.at[i], rf_r.at[i], right if way == 0 else left)

    def ring_start(L, b):
        i = L.l * nb + b

        @pl.when(home)
        def _():
            dst = hv.at[b, pl.ds(pl.multiple_of(x * blk + sl, sl), sl), :]
            rc(hs.at[b], dst, ad_s.at[i], ad_r.at[i], other).wait_recv()

        @pl.when(away)
        def _():
            for cc in range(2):
                dst = hv.at[b, pl.ds(pl.multiple_of(x * blk + cc * sl, sl), sl), :]
                rc(hs.at[b], dst, ax_s.at[i], ax_r.at[2 * i + cc], other).wait_recv()
        for way in range(2):
            ring(L, b, way).start()

    def ring_pass(L, b):
        for way in range(2):
            ring_in(L, b, way).wait_recv()
            ring2(L, b, way, xl if way == 0 else xr).start()

    def ring_end(L, b):
        for way in range(2):
            ring2(L, b, way, xo).wait_recv()

    def gather_sends_done(L, b):
        ax(L, b).wait_send()

        @pl.when(away)
        def _():
            ad(L, b).wait_send()
        for way in range(2):
            ring(L, b, way).wait_send()
            ring2(L, b, way, xl if way == 0 else xr).wait_send()

    def p_qkv(b):
        def step(i, _):
            col = hw * (1 - i) + 3 * hw * lax.div(i, 2)
            w = wv[lax.div(i, 2), :, cols(lax.rem(i, 2) * hw, hw)]
            qkv[b, :, cols(col, hw)] = jnp.dot(hv[b], w, preferred_element_type=F32).astype(BF)
            return 0
        lax.fori_loop(0, 3, step, 0)

    def p_gu(b, slot, k):
        acc = jnp.dot(hv[b], wv[slot], preferred_element_type=F32)
        g = acc[:, 0:hw].astype(BF).astype(F32)
        up = acc[:, hw:cw].astype(BF).astype(F32)
        om[b, :, cols(qw + hw * k, hw)] = (g * (1.0 / (1.0 + jnp.exp(-g))) * up).astype(BF)

    def attention(b):
        tq = 256
        kl = kcur[b, 0:1, 0:1]
        for i in range(seq // tq):
            n = tq * (i + 1)
            row = lax.broadcasted_iota(jnp.int32, (tq, n), 0) + tq * i
            col = lax.broadcasted_iota(jnp.int32, (tq, n), 1)
            ok = jnp.logical_and(col <= row, col < kl)

            def head(h, _):
                hc = pl.ds(pl.multiple_of(h * hd, hd), hd)
                qh = qkv[b, tq * i:tq * (i + 1), hc]
                s = lax.dot_general(qh, qkv[b, 0:n, kv0:kv0 + hd], (((1,), (1,)), ((), ())), preferred_element_type=F32) * hd ** -0.5
                s = jnp.where(ok, s, NEG_BIG)
                e = jnp.exp(s - jnp.max(s, axis=-1, keepdims=True))
                tot = jnp.sum(e, axis=-1, keepdims=True)
                o = jnp.dot(e.astype(BF), qkv[b, 0:n, kv0 + hd:kv0 + 2 * hd], preferred_element_type=F32)
                om[b, tq * i:tq * (i + 1), hc] = (o / tot).astype(BF)
                return 0

            lax.fori_loop(0, qw // hd, head, 0)

    def zblk(slot, xx, lo, n):
        return zs.at[slot, pl.ds(pl.multiple_of(xx * blk, blk), blk), pl.ds(lo, n)]

    def a_send(slot, way):
        return rc(zblk(slot, xo, way * hw, hw), ra.at[slot, way], a_s.at[2 * slot + way], a_r.at[2 * slot + way], right if way == 0 else left)

    def b_send(slot, way):
        return rc(zblk(slot, xr if way == 0 else xl, 0, cw), rb.at[slot, way], b_s.at[2 * slot + way], b_r.at[2 * slot + way],
                  right if way == 0 else left)

    def z_step(b, wref, j):
        slot = lax.rem(j, NS)

        @pl.when(j >= NS)
        def _():
            for way in range(2):
                a_send(slot, way).wait_send()
                b_send(slot, way).wait_send()
        zs[slot] = jnp.dot(om[b], wref[0:rw, :], preferred_element_type=F32).astype(BF)
        for way in range(2):
            a_send(slot, way).start()

    def rs_b(j):
        slot = lax.rem(j, NS)
        for way in range(2):
            a_send(slot, way).wait_recv()
            r = pl.ds(pl.multiple_of((xr if way == 0 else xl) * blk, blk), blk)
            cc = pl.ds(way * hw, hw)
            zs[slot, r, cc] = (zs[slot, r, cc].astype(F32) + ra[slot, way].astype(F32)).astype(BF)
        for way in range(2):
            b_send(slot, way).start()

    def c_send(L, b, n, slot, cc, inside):
        i = (L.l * n_t + n) * nb + b
        sem = c_s.at[2 * slot + cc]
        if inside:
            return rc(cst.at[slot, pl.ds(cc * sl, sl), :], parts.at[0, b, :, cols(n * cw, cw)], sem, pd_r.at[i], other)
        return rc(cst.at[slot, pl.ds(cc * sl, sl), :], parts.at[1, b, :, cols(n * cw, cw)], sem, pa_r.at[i], dev(L.q, x, cc))

    def c_wait(L, slot):
        @pl.when(away)
        def _():
            for cc in range(2):
                c_send(L, 0, 0, slot, cc, False).wait_send()

        @pl.when(home)
        def _():
            c_send(L, 0, 0, slot, 1, True).wait_send()

    def rs_c(L, j, b, t):
        slot, cslot = lax.rem(j, NS), lax.rem(j, NC)
        n = z_col(L, t)
        for way in range(2):
            b_send(slot, way).wait_recv()

        @pl.when(j >= NC)
        def _():
            c_wait(L, cslot)
        r = pl.ds(pl.multiple_of(x * blk, blk), blk)
        cst[cslot] = (zs[slot, r, :].astype(F32) + rb[slot, 0].astype(F32) + rb[slot, 1].astype(F32)).astype(BF)

        @pl.when(home)
        def _():
            c_send(L, b, n, cslot, 1, True).start()
            parts[0, b, :, cols(n * cw, cw)] = cst[cslot, 0:sl, :]

        @pl.when(away)
        def _():
            for cc in range(2):
                c_send(L, b, n, cslot, cc, False).start()

    def combine(L, b):
        for n in range(n_t):
            c_send(L, b, n, 0, 0, False).wait_recv()

            @pl.when(away)
            def _():
                c_send(L, b, n, 0, 0, True).wait_recv()

        def tile(i, _):
            r = pl.ds(pl.multiple_of(i * rows, rows), rows)
            z = parts[0, b, r, :].astype(F32) + parts[1, b, r, :].astype(F32)
            xv[b, r, :] = (xv[b, r, :].astype(F32) + z).astype(BF)
            return 0

        lax.fori_loop(0, sl // rows, tile, 0)

    L0, L1 = lays
    g_to = [dev(nbr1, x, c), dev(nbr3, x, c), dev(opp, x, c)]

    def gsl(e):
        return gfull.at[:, pl.ds(pl.multiple_of(e * dloc, dloc), dloc)]

    for i in range(3):
        rc(gain_ref, gsl(d), g_s.at[i], g_r.at[i], g_to[i]).start()

    @pl.when(away)
    def _():
        for l, L in enumerate(lays):
            rc(kl_ref, klb.at[l], k_s.at[l], k_r.at[l], dev(L.q, x, 1)).start()
    gfull[:, pl.ds(pl.multiple_of(d * dloc, dloc), dloc)] = gain_ref[...]

    def set_len(L):
        @pl.when(home)
        def _():
            kcur[...] = kl_ref[...]

        @pl.when(away)
        def _():
            rc(kl_ref, klb.at[L.l], k_s.at[L.l], k_r.at[L.l], other).wait_recv()
            kcur[...] = klb[L.l]

    def loop(n, fn, start=0):
        def body(i, _):
            fn(i)
            return 0
        lax.fori_loop(start, n, body, 0)

    def both(*conds):
        r = conds[0]
        for q in conds[1:]:
            r = jnp.logical_and(r, q)
        return r

    xload.wait()
    for i, e in enumerate((nbr1, nbr3, opp)):
        rc(gain_ref, gsl(e), g_s.at[i], g_r.at[i], g_to[i]).wait_recv()
    loop(n_in, lambda s: send_own(unit_in(L0, s), 'a'))
    layer_norm(L0, 0)
    share(L0, 0)
    layer_norm(L0, 1)
    loop(2, lambda s: send_own(unit_in(L0, s), 'b'))
    share(L0, 1)
    loop(n_in, lambda s: send_own(unit_in(L0, s), 'b'), 2)
    loop(n_out, lambda v: send_own(unit_out(L0, v), 'b'))
    set_len(L0)

    def in_ready(L, s):
        u = unit_in(L, s)
        fwd2(u)
        got1(u)
        got2(u)

    def fa(L, s):
        fwd1(unit_in(L, s), 'a')

    def fb(L, s):
        fwd1(unit_in(L, s), 'b')

    ring_start(L0, 0)
    for s in range(3):
        fa(L0, s)

    @pl.when(home)
    def _():
        ring_pass(L0, 0)
    fb(L0, 0)
    fb(L0, 1)
    fa(L0, 3)

    @pl.when(away)
    def _():
        ring_pass(L0, 0)
    fa(L0, 4)
    ring_start(L0, 1)
    fwd2(unit_in(L0, 0))
    fa(L0, 5)
    fb(L0, 2)
    fwd2(unit_in(L0, 1))
    ring_end(L0, 0)
    n_early = 2

    def stage0(b):
        first = b == 0

        @pl.when(first)
        def _():
            for s in range(2):
                got1(unit_in(L0, s))
                got2(unit_in(L0, s))

        @pl.when(jnp.logical_not(first))
        def _():
            fb(L0, 7)
            ring_end(L0, 1)
        load_in(unit_in(L0, 0), 0)
        load_in(unit_in(L0, 1), 1)
        wait_in(0, cw)
        wait_in(1, hw)
        p_qkv(b)

        @pl.when(first)
        def _():
            fb(L0, 3)
        attention(b)

        @pl.when(first)
        def _():
            fb(L0, 4)
            fa(L0, 6)
            in_ready(L0, 2)

        @pl.when(jnp.logical_not(first))
        def _():
            fb(L0, 8)
            fa(L0, 8)
        load_in(unit_in(L0, 2), 0)

        def gu(k):
            slot = lax.rem(k, 2)
            wait_in(slot, cw)
            p_gu(b, slot, k)

            @pl.when(both(first, k == 0))
            def _():
                fb(L0, 5)
                ring_pass(L0, 1)
                fb(L0, 6)
                fa(L0, 7)
                in_ready(L0, 3)

            @pl.when(both(jnp.logical_not(first), k == 0))
            def _():
                fwd2(unit_in(L0, 4))

            @pl.when(k + 1 < n_early)
            def _():
                load_in(unit_in(L0, k + 3), 1 - slot)
        loop(n_early, gu)

    loop(nb, stage0)
    fb(L0, 9)
    u4 = unit_in(L0, n_early + 2)
    got1(u4)
    got2(u4)
    load_in(u4, n_early % 2)

    def gu0(k):
        s = k + 2
        slot = lax.rem(k, 2)
        wait_in(slot, cw)
        p_gu(0, slot, k)

        @pl.when(k == n_early)
        def _():
            fa(L0, 9)

        @pl.when(both(k >= n_gu - 1 - n_out, k < n_gu - 1))
        def _():
            fwd1(unit_out(L0, k - (n_gu - 1 - n_out)), 'b')

        @pl.when(k == n_gu // 2)
        def _():
            loop(n_out, lambda v: send_own(unit_out(L0, v), 'a'))

        @pl.when(s + 1 < n_in)
        def _():
            in_ready(L0, s + 1)
            load_in(unit_in(L0, s + 1), 1 - slot)

        @pl.when(s + 1 == n_in)
        def _():
            out_arrives(L0, 0)
            load_out(L0, 0, *wslot_of(1 - slot))
        p_gu(1, slot, k)

        @pl.when(both(k >= n_gu - 4, k < n_gu - 2))
        def _():
            for i in range(2):
                send_own(unit_in(L1, 2 * (k - (n_gu - 4)) + i), 'a')

        @pl.when(k >= n_gu - 2)
        def _():
            send_own(unit_in(L1, k - (n_gu - 2) + 4), 'a')

    loop(n_gu, gu0, n_early)
    for b in range(nb):
        gather_sends_done(L0, b)

    @pl.when(away)
    def _():
        for cc in range(2):
            pl.semaphore_signal(free_sem, inc=1, device_id=dev(L1.q, x, cc), device_id_type=MESH)
    z0 = n_gu % 2
    j_end = nb * n_t
    j_late = j_end // 2

    assert nb == 2 and n_t == 8

    def pick(i, values):
        r = values[-1]
        for k in range(len(values) - 1):
            r = jnp.where(i == k, values[k], r)
        return r

    def jt(j):
        late, r = lax.div(j, j_late), lax.rem(j, j_late)
        b = (1 - late) * lax.rem(r, nb) + late * pick(r, (0, 0, 1, 0, 0, 1, 1, 1))
        t = (1 - late) * lax.div(r, nb) + late * (n_t // 2 + pick(r, (0, 1, 0, 2, 3, 1, 2, 3)))
        return b, t

    def z_loop0(j):
        slot = lax.rem(j + z0, 2)
        b, t = jt(j)
        wait_out(*wslot_of(slot))
        z_step(b, wv.at[slot], j)

        @pl.when(j + 1 < j_end)
        def _():
            b1, t1 = jt(j + 1)

            @pl.when(b1 == 0)
            def _():
                out_arrives(L0, t1)
            load_out(L0, t1, *wslot_of(1 - slot))

        @pl.when(j >= 1)
        def _():
            rs_b(j - 1)

        @pl.when(j >= 2)
        def _():
            b2, t2 = jt(j - 2)
            rs_c(L0, j - 2, b2, t2)
        half = lax.div(j, 2)

        @pl.when(both(lax.rem(j, 2) == 1, half + 6 < n_in))
        def _():
            send_own(unit_in(L1, half + 6), 'a')

        @pl.when(lax.rem(j, 2) == 1)
        def _():
            fa(L1, half)

        @pl.when(j == j_late)
        def _():
            send_own(unit_out(L1, 0), 'a')

        @pl.when(both(j >= j_end - 6, lax.rem(j, 2) == 0, j < j_end - 2))
        def _():
            for i in range(2):
                send_own(unit_in(L1, j - (j_end - 6) + i), 'b')

    loop(j_end, z_loop0)
    pl.semaphore_wait(free_sem, 1)
    combine(L0, 0)
    layer_norm(L1, 0)
    share(L1, 0)
    rs_b(j_end - 1)
    rs_c(L0, j_end - 2, nb - 1, n_t - 2)
    rs_c(L0, j_end - 1, nb - 1, n_t - 1)

    @pl.when(home)
    def _():
        ring_start(L1, 0)
    for s in range(3):
        fb(L1, s)
    combine(L0, 1)
    layer_norm(L1, 1)
    share(L1, 1)
    send_own(unit_in(L1, 4), 'b')
    loop(n_in, lambda s: send_own(unit_in(L1, s), 'b'), 5)
    loop(n_out, lambda v: send_own(unit_out(L1, v), 'b'))
    loop(n_in, lambda s: fa(L1, s), n_in - 2)
    set_len(L1)

    @pl.when(away)
    def _():
        ring_start(L1, 0)
    fb(L1, 3)
    in_ready(L1, 0)
    load_in(unit_in(L1, 0), 0)
    in_ready(L1, 1)
    load_in(unit_in(L1, 1), 1)

    @pl.when(home)
    def _():
        ring_pass(L1, 0)
    fwd2(unit_in(L1, 2))
    send_own(unit_out(L1, 1), 'a')
    fb(L1, 4)

    @pl.when(away)
    def _():
        ring_pass(L1, 0)
        ring_start(L1, 1)
    fb(L1, 5)
    fwd2(unit_in(L1, 3))
    fb(L1, 6)
    fwd2(unit_in(L1, 4))
    assert n_gu == n_t

    n_lead = 2

    def z_next(t):
        @pl.when(t < n_t)
        def _():
            out_arrives(L1, t)
            load_out(L1, t, wz, wzs.at[0])

    def z_early(t):
        wait_out(wz, wzs.at[0])
        z_step(0, wz, j_end + t)
        if t:
            rs_b(j_end + t - 1)
        z_next(t + 1)

    def stage1(b):
        first = b == 0

        @pl.when(jnp.logical_not(first))
        def _():
            load_in(unit_in(L1, 0), 0)
            load_in(unit_in(L1, 1), 1)
            fwd1(unit_out(L1, 1), 'b')
            z_early(0)
        ring_end(L1, b)
        wait_in(0, cw)
        wait_in(1, hw)
        p_qkv(b)

        @pl.when(first)
        def _():
            fb(L1, 7)
            fwd2(unit_in(L1, 5))
            got1(unit_in(L1, 2))
            got2(unit_in(L1, 2))

        @pl.when(both(first, home))
        def _():
            ring_start(L1, 1)
        load_in(unit_in(L1, 2), 0)

        @pl.when(jnp.logical_not(first))
        def _():
            z_early(1)
        attention(b)

        @pl.when(first)
        def _():
            fb(L1, 8)
            fwd2(unit_in(L1, 6))

        def gu(k):
            slot = lax.rem(k, 2)

            @pl.when(both(first, k == 0))
            def _():
                fb(L1, n_in - 1)

            @pl.when(both(first, k + 7 < n_in))
            def _():
                fwd2(unit_in(L1, k + 7))

            @pl.when(both(first, k >= n_gu - n_out))
            def _():
                fwd1(unit_out(L1, k - (n_gu - n_out)), 'a')

            @pl.when(both(first, k == n_gu - 2))
            def _():
                fwd1(unit_out(L1, 0), 'b')

            @pl.when(both(jnp.logical_not(first), k >= n_lead, k < n_lead + n_out))
            def _():
                fwd2(unit_out(L1, k - n_lead))

            @pl.when(both(first, k + 1 < n_gu))
            def _():
                got1(unit_in(L1, k + 3))
                got2(unit_in(L1, k + 3))

            @pl.when(k + 1 < n_gu)
            def _():
                load_in(unit_in(L1, k + 3), 1 - slot)
            wait_in(slot, cw)
            p_gu(b, slot, k)

            @pl.when(both(first, k == 5))
            def _():
                ring_pass(L1, 1)

            j = j_end + n_lead + k
            later = jnp.logical_not(first)

            @pl.when(both(later, k + n_lead < n_t))
            def _():
                wait_out(wz, wzs.at[0])
                z_step(0, wz, j)

            @pl.when(both(later, k + n_lead <= n_t))
            def _():
                rs_b(j - 1)

            @pl.when(later)
            def _():
                rs_c(L1, j - 2, 0, k)

            @pl.when(later)
            def _():
                z_next(k + n_lead + 1)

            @pl.when(both(first, k == n_gu - 1))
            def _():
                z_next(0)
        loop(n_gu, gu)

    loop(nb, stage1)
    load_out(L1, 0, *wslot_of(0))
    for b in range(nb):
        gather_sends_done(L1, b)

    def z_loop1(t):
        wslot = lax.rem(t, 2)
        wait_out(*wslot_of(wslot))

        @pl.when(t + 1 < n_t)
        def _():
            load_out(L1, t + 1, *wslot_of(1 - wslot))
        j = j_end + n_t + t
        z_step(1, wv.at[wslot], j)

        @pl.when(t >= 1)
        def _():
            rs_b(j - 1)

        @pl.when(t >= 2)
        def _():
            rs_c(L1, j - 2, 1, t - 2)

    loop(n_t, z_loop1)
    j_last = 2 * j_end - 1
    rs_b(j_last)
    rs_c(L1, j_last - 1, 1, n_t - 2)
    rs_c(L1, j_last, 1, n_t - 1)
    for b in range(nb):
        combine(L1, b)
    yout = pltpu.make_async_copy(xv, y_ref, misc.at[0])
    yout.start()

    def layer_sends_done(L):
        loop(n_in, lambda s: sends_done(unit_in(L, s)))
        loop(n_out, lambda v: sends_done(unit_out(L, v)))

    layer_sends_done(L0)
    layer_sends_done(L1)
    for i in range(3):
        rc(gain_ref, gsl(d), g_s.at[i], g_r.at[i], g_to[i]).wait_send()

    @pl.when(away)
    def _():
        for l in range(nl):
            rc(kl_ref, klb.at[l], k_s.at[l], k_r.at[l], other).wait_send()
    for slot in range(NC):
        c_wait(L1, slot)
    for slot in range(NS):
        for way in range(2):
            a_send(slot, way).wait_send()
            b_send(slot, way).wait_send()
    yout.wait()


def solution(mesh):
    n_data = mesh.shape['data']
    n_x = mesh.shape['model'] // 2
    batch_axes = ('rep', 'data')

    def device_step(x_loc, len_loc, gain_loc, w_in_loc, w_attn_loc, w_mlp_loc):
        nl, dloc, block_in = w_in_loc.shape
        qw, ff = w_attn_loc.shape[1], w_mlp_loc.shape[1]
        hd = (block_in - qw - 2 * ff) // 2
        nb, sl, dm = x_loc.shape
        seq = sl * 2 * n_x
        cfg = (n_data, n_x, nb, sl, dm, dloc, qw, hd, ff, nl)
        cw = 512
        n_u = 2 + ff // (cw // 2) + dloc // cw
        n_t = n_data * (dloc // cw)
        lens = jnp.broadcast_to(len_loc[:, None, None], (nb, 8, 128))
        gain = gain_loc.astype(F32)
        anyspec = pl.BlockSpec(memory_space=pl.ANY)
        vspec = pl.BlockSpec(memory_space=pltpu.VMEM)
        sem = pltpu.SemaphoreType.DMA
        out = pl.pallas_call(
            functools.partial(kernel, cfg),
            out_shape=[
                jax.ShapeDtypeStruct((nb, sl, dm), BF),
                jax.ShapeDtypeStruct((nl, n_data, dloc, block_in), BF),
                jax.ShapeDtypeStruct((nl, n_data, qw, dloc), BF),
                jax.ShapeDtypeStruct((nl, n_data, ff, dloc), BF),
            ],
            in_specs=[anyspec, vspec, vspec, anyspec, anyspec, anyspec],
            out_specs=[anyspec] * 4,
            scratch_shapes=[
                pltpu.VMEM((nb, seq, dm), BF),
                pltpu.VMEM((nb, seq, qw + 2 * hd), BF),
                pltpu.VMEM((nb, seq, qw + ff), BF),
                pltpu.VMEM((2, dm, cw), BF),
                pltpu.VMEM((qw + ff, cw), BF),
                pltpu.VMEM((NS, seq, cw), BF),
                pltpu.VMEM((NS, 2, 2 * sl, cw // 2), BF),
                pltpu.VMEM((NS, 2, 2 * sl, cw), BF),
                pltpu.VMEM((NC, 2 * sl, cw), BF),
                pltpu.VMEM((2, nb, sl, dm), BF),
                pltpu.VMEM((nb, sl, dm), BF),
                pltpu.VMEM((nb, sl, dm), BF),
                pltpu.VMEM((nl, dm), F32),
                pltpu.VMEM((nl, nb, 8, 128), jnp.int32),
                pltpu.VMEM((nb, 8, 128), jnp.int32),
            ] + [sem((nl * n_u * 2,))] * 8 + [
                sem((2,)),
                sem((1,)),
                sem((1,)),
                sem((3,)), sem((3,)),
                sem((nl,)), sem((nl,)),
                sem((nl * nb,)), sem((nl * nb * 2,)),
                sem((nl * nb,)), sem((nl * nb,)),
                sem((nl * nb * 2,)), sem((nl * nb * 2,)),
                sem((nl * nb * 2,)), sem((nl * nb * 2,)),
                sem((NS * 2,)), sem((NS * 2,)), sem((NS * 2,)), sem((NS * 2,)), sem((NC * 2,)),
                sem((nl * n_t * nb,)), sem((nl * n_t * nb,)),
                pltpu.SemaphoreType.REGULAR,
            ],
            compiler_params=pltpu.CompilerParams(collective_id=0, has_side_effects=True, vmem_limit_bytes=63 * 1024 * 1024),
        )(x_loc, lens, gain, w_in_loc, w_attn_loc, w_mlp_loc)
        return out[0]

    return jax.shard_map(device_step, mesh=mesh, in_specs=(P(batch_axes, 'model', None), P(batch_axes), P(None, 'data'), P(None, 'data', 'model'), P(None, 'model', 'data'), P(None, 'model', 'data')), out_specs=P(batch_axes, 'model', None), check_vma=False)
```
